128 devices in a mesh: tok: 16 (over x, y_lo, core), col: 8 (over y_hi, z).
Axes of the slice: x: 4, y: 4 (y_hi: 2, y_lo: 2; y = y_hi * 2 + y_lo), z: 4, core: 2. Of those that a mesh axis runs over, the one named last changes fastest.
Arguments:
- activations: bfloat16 [2, 24576, 4096], P(None, 'tok', 'col'), may hold values from -6 to 6
- out_grads: bfloat16 [2, 24576, 4096], P(None, 'tok', 'col'), may hold values from -0.059814453 to 0.059814453
- token_mask: int32 [2, 24576], P(None, 'tok'), may hold values 0 or 1
- row_signs: int32 [4096], P('tok'), may hold values from 0 to 1
- col_signs: int32 [4096], P('col'), may hold values from 0 to 1
- bank: float32 [16, 4096, 4096], P(None, 'tok', 'col'), may hold values from -6 to 6
- bank_index: int32 [2], replicated, may hold values from 0 to 15, as said below
Outputs:
- fingerprints: float32 [2, 4096, 4096], P(None, 'tok', 'col')
- scores: float32 [2], replicated
The draws below stay inside these ranges and needn't reach their ends.
Inputs may be any that keep to these rules, and one draw needn't show every extreme that they name: `bank_index`: the 2 values are distinct, and one of them is 15.
All inputs are finite; a program needn't handle non-finite values. No bound on the sum of `token_mask` on one device may be relied on, other than what follows from the above.
Results may differ from the reference program's by a relative error of at most 0.0003.
Values may be sent and summed in bfloat16 or wider, within the bound.
A program may use at most 128 MiB of HBM per device.

```python
import math
import jax
import jax.numpy as jnp
from jax import lax

D = 4096
SEQS = 2
BANK = 16
TOKENS = 24576


def draw_bank_index(key, part):
    order = jax.random.permutation(jax.random.fold_in(key, 7), BANK - 1)[:SEQS].astype(jnp.int32)
    position = jax.random.randint(jax.random.fold_in(key, 11), (), 0, SEQS)
    slots = jnp.arange(SEQS, dtype=jnp.int32)
    return jnp.where(slots == position, BANK - 1, order).astype(jnp.int32)


def place_ends(array, own_key, smallest, top_value):
    extent = array.shape
    spot = [jax.random.randint(jax.random.fold_in(own_key, axis), (), 0, extent[axis]) for axis in range(len(extent))]
    array = array.at[tuple(spot)].set(smallest)
    longest = extent.index(max(extent))
    spot[longest] = (spot[longest] + 1) % extent[longest]
    return array.at[tuple(spot)].set(top_value)


def shard_levels(rng, shape, pieces, least, top_value):
    level = 1.0
    for dim, shards_of in pieces:
        draws = jax.random.uniform(jax.random.fold_in(jax.random.fold_in(rng, 6), dim), (shards_of,), jnp.float32, least / len(pieces), top_value / len(pieces))
        level = level * jnp.repeat(jnp.exp(draws), shape[dim] // shards_of).reshape((-1,) + (1,) * (len(shape) - 1 - dim))
    return level


def noise(key, extent, scale, reach, pieces=(), kind=jnp.bfloat16):
    result = scale * jax.random.normal(key, extent, jnp.float32)
    if pieces:
        result = result * shard_levels(key, extent, pieces, -0.22, 0.18)
    return jnp.clip(result, -reach, reach).astype(kind)


def setup_inputs(seed: int = 0) -> dict:
    key_of = jax.random.split(jax.random.key(seed), 8)
    return {
        "activations": noise(key_of[0], (SEQS, TOKENS, D), 1.0, 6.0, ((1, 16), (2, 8))),
        "out_grads": noise(key_of[1], (SEQS, TOKENS, D), 0.01, 0.059814453, ((1, 16), (2, 8))),
        "token_mask": place_ends((jax.random.randint(key_of[2], (SEQS, TOKENS), 0, 4) < 3).astype(jnp.int32), jax.random.fold_in(key_of[2], 1), 0, 1),
        "row_signs": place_ends(jax.random.randint(key_of[3], (D,), 0, 2), jax.random.fold_in(key_of[3], 1), 0, 1).astype(jnp.int32),
        "col_signs": place_ends(jax.random.randint(key_of[4], (D,), 0, 2), jax.random.fold_in(key_of[4], 1), 0, 1).astype(jnp.int32),
        "bank": noise(key_of[5], (BANK, D, D), 1.0, 6.0, ((1, 16), (2, 8)), jnp.float32),
        "bank_index": draw_bank_index(jax.random.fold_in(key_of[7], 71), 0),
    }


HIGH = lax.Precision.HIGHEST

def hadamard(order):
    positions = jnp.arange(order, dtype=jnp.int32)
    common_bits = jnp.bitwise_and(positions[:, None], positions[None, :])
    parity = jnp.zeros((order, order), jnp.int32)
    for bit_number in range(max(order.bit_length() - 1, 0)):
        parity = parity + jnp.bitwise_and(jnp.right_shift(common_bits, bit_number), 1)
    return (1 - 2 * (parity % 2)).astype(jnp.float32)

def mix_rows(matrix):
    first = 2 ** ((D.bit_length() - 1) // 2)
    second = D // first
    blocks = matrix.reshape(first, second, matrix.shape[1])
    blocks = jnp.einsum('ab,bqm->aqm', hadamard(first), blocks, precision=HIGH)
    blocks = jnp.einsum('qr,arm->aqm', hadamard(second), blocks, precision=HIGH)
    return blocks.reshape(D, matrix.shape[1]) / math.sqrt(D)

def reference(activations, out_grads, token_mask, row_signs, col_signs, bank, bank_index):
    row_pm = (2 * row_signs - 1).astype(jnp.float32)
    col_pm = (2 * col_signs - 1).astype(jnp.float32)
    prints = []
    scores = []
    squared = float(D) * float(D)
    for seq_number in range(SEQS):
        masked = out_grads[seq_number] * token_mask[seq_number][:, None].astype(jnp.bfloat16)
        gradient = jnp.dot(activations[seq_number].T, masked, preferred_element_type=jnp.float32)
        signed = gradient * row_pm[:, None] * col_pm[None, :]
        rows_done = mix_rows(signed)
        finished = mix_rows(rows_done.T).T
        chosen = lax.dynamic_index_in_dim(bank, bank_index[seq_number], 0, keepdims=False)
        cross = jnp.sum(finished * chosen)
        own = jnp.sum(finished * finished)
        refsq = jnp.sum(chosen * chosen)
        score = D * (cross / squared) / jnp.sqrt((own / squared + 1e-06) * (refsq / squared + 1e-06))
        prints.append(finished)
        scores.append(score)
    return (jnp.stack(prints), jnp.stack(scores))
```

```python
import functools
import math

import jax
import jax.numpy as jnp
from jax import lax
from jax.experimental import pallas as pl
from jax.experimental.pallas import tpu as pltpu
from jax.sharding import Mesh
from jax.sharding import PartitionSpec as P

D = 4096
TOK = ("tok_0", "tok_1", "tok_2")
COL = ("col_0", "col_1")
EVERY = ("tok_0", "tok_1", "tok_2", "col_0", "col_1")
HIGH = lax.Precision.HIGHEST
MESH = pl.DeviceIdType.MESH

SEQS = 2
TOKENS = 1536
HALF = TOKENS // 2
FEATS = 512
BLOCKS = 4
UNITS = SEQS * BLOCKS


def hadamard(order):
    positions = jnp.arange(order, dtype=jnp.int32)
    common_bits = jnp.bitwise_and(positions[:, None], positions[None, :])
    parity = jnp.zeros((order, order), jnp.int32)
    for bit_number in range(max(order.bit_length() - 1, 0)):
        parity = parity + jnp.bitwise_and(jnp.right_shift(common_bits, bit_number), 1)
    return (1 - 2 * (parity % 2)).astype(jnp.float32)


def gather_kernel(
    acts,
    grads,
    tables,
    out,
    a_buf,
    m_buf,
    relay,
    turned,
    part,
    core_in,
    x_half,
    x_full,
    y_in,
    load_sem,
    a_send,
    a_recv,
    m_send,
    m_recv,
    core_send,
    core_recv,
    xh_send,
    xh_recv,
    xf_send,
    xf_recv,
    y_send,
    y_recv,
):
    x = lax.axis_index("tok_0")
    y_lo = lax.axis_index("tok_1")
    core = lax.axis_index("tok_2")
    y_hi = lax.axis_index("col_0")
    z = lax.axis_index("col_1")
    y = y_hi * 2 + y_lo

    def at_y(value):
        value = lax.rem(value, 4)
        return (x, lax.rem(value, 2), core, lax.div(value, 2), z)

    x_next, x_prev, x_far = lax.rem(x + 1, 4), lax.rem(x + 3, 4), lax.rem(x + 2, 4)
    z_ids = ((x, y_lo, core, y_hi, lax.rem(z + 1, 4)), (x, y_lo, core, y_hi, lax.rem(z + 3, 4)))
    y_ids = (at_y(y + 1), at_y(y + 3))
    x_ids = ((x_next, y_lo, core, y_hi, z), (x_prev, y_lo, core, y_hi, z))
    core_id = (x, y_lo, 1 - core, y_hi, z)
    pair_id = (x, 1 - y_lo, core, y_hi, z)

    loads = []
    for seq in range(SEQS):
        loads.append(pltpu.make_async_copy(acts.at[seq], a_buf.at[seq, 0], load_sem.at[2 * seq]))
        loads.append(pltpu.make_async_copy(grads.at[seq], m_buf.at[seq, 0], load_sem.at[2 * seq + 1]))
    for copy in loads:
        copy.start()

    barrier = pltpu.get_barrier_semaphore()
    partners = (*z_ids, *y_ids, *x_ids, core_id)
    for partner in partners:
        pl.semaphore_signal(barrier, inc=1, device_id=partner, device_id_type=MESH)
    pl.semaphore_wait(barrier, len(partners))

    def rows_of(half):
        return pl.ds(half * HALF, HALF)

    def remote(src, dst, send, recv, device):
        return pltpu.make_async_remote_copy(
            src_ref=src, dst_ref=dst, send_sem=send, recv_sem=recv, device_id=device, device_id_type=MESH
        )

    def ring_copy(seq, way, half, hop):
        slot = (3, 1)[way] if hop == 0 else 2
        index = (seq * 2 + way) * 3 + (2 if hop else half)
        src = acts.at[seq, rows_of(half)] if hop == 0 else a_buf.at[seq, (3, 1)[way], rows_of(half)]
        return remote(src, a_buf.at[seq, slot, rows_of(half)], a_send.at[index], a_recv.at[index], z_ids[way])

    def swap_copy(seq, way, hop):
        index = (seq * 2 + way) * 2 + hop
        src = relay.at[seq, way] if hop else grads.at[seq, rows_of(way)]
        dst = m_buf.at[seq, 1, rows_of(way)] if hop else relay.at[seq, way]
        return remote(src, dst, m_send.at[index], m_recv.at[index], y_ids[way])

    sent = []

    def start(copy):
        copy.start()
        sent.append(copy)

    def ring_own(seq):
        for step in range(2):
            for way in range(2):
                start(ring_copy(seq, way, (way + step) % 2, 0))

    def ring_pass(seq):
        for way in range(2):
            ring_copy(seq, way, way, 0).wait_recv()
            start(ring_copy(seq, way, way, 1))

    def swap_own(seq):
        for way in range(2):
            start(swap_copy(seq, way, 0))

    def swap_pass(seq):
        for way in range(2):
            swap_copy(seq, way, 0).wait_recv()
            start(swap_copy(seq, way, 1))

    def swap_end(seq):
        for way in range(2):
            swap_copy(seq, way, 1).wait_recv()

    def ring_near(seq, way):
        ring_copy(seq, way, 1 - way, 0).wait_recv()

    def ring_far(seq):
        for way in range(2):
            ring_copy(seq, way, way, 1).wait_recv()

    core_sign = (1 - 2 * core).astype(jnp.float32)

    def compute(unit, seq, slot):
        block = lax.rem(z + slot, 4)

        @pl.loop(0, 2)
        def _(b):
            columns = pl.ds(pl.multiple_of(b * 256, 256), 256)
            turned[b] = a_buf[seq, slot, :, columns].T

        @pl.loop(0, 4)
        def _(i):
            b = lax.div(i, 2)
            m = lax.rem(i, 2)
            tile = jnp.dot(turned[b], m_buf[seq, m], preferred_element_type=jnp.float32)
            coarse = tile.astype(jnp.bfloat16)
            fine = (tile - coarse.astype(jnp.float32)).astype(jnp.bfloat16)
            table = tables[2 * block + b]
            mixed = jnp.dot(table, coarse, preferred_element_type=jnp.float32)
            mixed += jnp.dot(table, fine, preferred_element_type=jnp.float32)
            columns = pl.ds(pl.multiple_of(lax.rem(m + y_hi, 2) * 512, 512), 512)
            part[unit, b, :, columns] = mixed

        @pl.loop(0, 32)
        def _(i):
            rows = pl.ds(pl.multiple_of(i * 8, 8), 8)
            low = part[unit, 0, rows]
            high = part[unit, 1, rows] * core_sign
            part[unit, 0, rows] = low + high
            part[unit, 1, rows] = low - high

        start(core_copy(unit))

    def core_copy(unit):
        return remote(part.at[unit, 1], core_in.at[unit], core_send.at[unit], core_recv.at[unit], core_id)

    def chunk(unit, x_of):
        return part.at[unit, 0, pl.ds(pl.multiple_of(x_of * 64, 64), 64)]

    def x_half_copy(unit, way):
        rows = pl.ds(pl.multiple_of(x_far * 64 + way * 32, 32), 32)
        index = unit * 2 + way
        return remote(
            part.at[unit, 0, rows], x_half.at[unit, way], xh_send.at[index], xh_recv.at[index], x_ids[way]
        )

    def x_full_copy(unit, way):
        index = unit * 2 + way
        src = chunk(unit, (x_next, x_prev)[way])
        return remote(src, x_full.at[unit, way], xf_send.at[index], xf_recv.at[index], x_ids[way])

    def y_copy(unit):
        rows = pl.ds(pl.multiple_of(x * 64 + (1 - y_lo) * 32, 32), 32)
        return remote(part.at[unit, 0, rows], y_in.at[unit], y_send.at[unit], y_recv.at[unit], pair_id)

    def sum_core(unit):
        core_copy(unit).wait_recv()

        def add(first, rows):
            @pl.loop(0, rows // 8)
            def _(i):
                there = pl.ds(pl.multiple_of(first + i * 8, 8), 8)
                part[unit, 0, there] += core_in[unit, there]

        add(x_far * 64, 64)
        for way in range(2):
            start(x_half_copy(unit, way))
        for other in (x_next, x_prev, x):
            add(other * 64, 64)

    def sum_half(unit):
        for way in range(2):
            x_half_copy(unit, way).wait_recv()
            first = (x_next, x_prev)[way] * 64 + way * 32

            @pl.loop(0, 4)
            def _(i):
                there = pl.ds(pl.multiple_of(first + i * 8, 8), 8)
                part[unit, 0, there] += x_half[unit, way, pl.ds(pl.multiple_of(i * 8, 8), 8)]

            start(x_full_copy(unit, way))

    def sum_full(unit):
        for way in range(2):
            x_full_copy(unit, way).wait_recv()

        @pl.loop(0, 8)
        def _(i):
            there = pl.ds(pl.multiple_of(x * 64 + i * 8, 8), 8)
            here = pl.ds(pl.multiple_of(i * 8, 8), 8)
            part[unit, 0, there] += x_full[unit, 0, here] + x_full[unit, 1, here]

        start(y_copy(unit))

    def finish(unit, seq, slot):
        block = lax.rem(z + slot, 4)
        y_copy(unit).wait_recv()

        @pl.loop(0, 4)
        def _(i):
            here = pl.ds(pl.multiple_of(i * 8, 8), 8)
            there = pl.ds(pl.multiple_of(x * 64 + y_lo * 32 + i * 8, 8), 8)
            out[seq, block, here] = part[unit, 0, there] + y_in[unit, here]

    order = [(seq, slot) for seq in range(SEQS) for slot in (0, 3, 1, 2)]
    run = [functools.partial(compute, unit, *order[unit]) for unit in range(UNITS)]
    end = [functools.partial(finish, unit, *order[unit]) for unit in range(UNITS)]

    ring_own(0)
    swap_own(0)
    swap_pass(0)
    swap_own(1)
    ring_pass(0)
    ring_own(1)
    for copy in loads:
        copy.wait()
    swap_end(0)
    run[0]()
    ring_near(0, 0)
    run[1]()
    sum_core(0)
    ring_near(0, 1)
    run[2]()
    sum_core(1)
    sum_half(0)
    sum_core(2)
    sum_half(1)
    swap_pass(1)
    sum_full(0)
    sum_half(2)
    ring_far(0)
    run[3]()
    sum_core(3)
    sum_full(1)
    end[0]()
    sum_half(3)
    sum_full(2)
    end[1]()
    ring_pass(1)
    swap_end(1)
    run[4]()
    sum_core(4)
    sum_full(3)
    end[2]()
    sum_half(4)
    end[3]()
    sum_full(4)
    ring_near(1, 0)
    run[5]()
    ring_near(1, 1)
    run[6]()
    sum_core(5)
    sum_core(6)
    sum_half(5)
    sum_half(6)
    end[4]()
    sum_full(5)
    sum_full(6)
    ring_far(1)
    run[7]()
    sum_core(7)
    end[5]()
    end[6]()
    sum_half(7)
    sum_full(7)
    end[7]()
    for copy in sent:
        copy.wait_send()


def gathered_products(acts, grads, tables):
    dma = pltpu.SemaphoreType.DMA
    return pl.pallas_call(
        gather_kernel,
        out_shape=jax.ShapeDtypeStruct((SEQS, BLOCKS, 32, 2 * FEATS), jnp.float32),
        in_specs=[
            pl.BlockSpec(memory_space=pl.ANY),
            pl.BlockSpec(memory_space=pl.ANY),
            pl.BlockSpec(memory_space=pltpu.VMEM),
        ],
        out_specs=pl.BlockSpec(memory_space=pltpu.VMEM),
        scratch_shapes=[
            pltpu.VMEM((SEQS, BLOCKS, TOKENS, FEATS), jnp.bfloat16),
            pltpu.VMEM((SEQS, 2, TOKENS, FEATS), jnp.bfloat16),
            pltpu.VMEM((SEQS, 2, HALF, FEATS), jnp.bfloat16),
            pltpu.VMEM((2, 256, TOKENS), jnp.bfloat16),
            pltpu.VMEM((UNITS, 2, 256, 2 * FEATS), jnp.float32),
            pltpu.VMEM((UNITS, 256, 2 * FEATS), jnp.float32),
            pltpu.VMEM((UNITS, 2, 32, 2 * FEATS), jnp.float32),
            pltpu.VMEM((UNITS, 2, 64, 2 * FEATS), jnp.float32),
            pltpu.VMEM((UNITS, 32, 2 * FEATS), jnp.float32),
            dma((4,)),
            dma((12,)),
            dma((12,)),
            dma((8,)),
            dma((8,)),
            dma((UNITS,)),
            dma((UNITS,)),
            dma((2 * UNITS,)),
            dma((2 * UNITS,)),
            dma((2 * UNITS,)),
            dma((2 * UNITS,)),
            dma((UNITS,)),
            dma((UNITS,)),
        ],
        compiler_params=pltpu.CompilerParams(
            collective_id=0, has_side_effects=True, vmem_limit_bytes=67043328
        ),
    )(acts, grads, tables)


def body(activations, out_grads, token_mask, row_signs, col_signs, bank, bank_index):
    squared = float(D) * float(D)
    y_hi = lax.axis_index("col_0")
    all_signs = lax.all_gather(row_signs, TOK, axis=0, tiled=True)
    mine = lax.dynamic_slice_in_dim(all_signs, y_hi * 2048, 2048, 0)
    signs = (2 * mine - 1).astype(jnp.float32).reshape(8, 1, 256)
    tables = (hadamard(256)[None] * signs).astype(jnp.bfloat16)
    col_pm = (2 * col_signs - 1).astype(jnp.bfloat16)
    grads = out_grads * token_mask[:, :, None].astype(jnp.bfloat16) * col_pm[None, None, :]

    sums = gathered_products(activations, grads, tables)

    sums = jnp.einsum("am,sapc->smpc", hadamard(4), sums, precision=HIGH)
    sums = sums.reshape(SEQS, 4, 32, 2, 512)
    sums = jnp.einsum("yh,smpyc->smphc", hadamard(2), sums, precision=HIGH)
    sums = jnp.dot(sums, hadamard(512), precision=HIGH) * (1.0 / D)
    pieces = sums.reshape(SEQS, 4, 4, 8, 2, 512).transpose(4, 2, 0, 1, 3, 5).reshape(8, SEQS, 4, 8, 512)
    pieces = lax.all_to_all(pieces, COL, split_axis=0, concat_axis=0, tiled=True)
    pieces = jnp.einsum("ab,bsmpc->asmpc", hadamard(8), pieces, precision=HIGH)
    pieces = pieces.reshape(2, 4, SEQS, 4, 8, 512).transpose(0, 3, 1, 2, 4, 5).reshape(32, SEQS, 8, 512)
    pieces = lax.all_to_all(pieces, ("tok_0", "tok_1", "col_1"), split_axis=0, concat_axis=0, tiled=True)
    prints = pieces.transpose(1, 0, 2, 3).reshape(SEQS, 256, 512)

    chosen = jnp.stack(
        [lax.dynamic_index_in_dim(bank, bank_index[seq], 0, keepdims=False) for seq in range(SEQS)]
    )
    totals = jnp.concatenate(
        [
            jnp.sum(prints * chosen, axis=(1, 2)),
            jnp.sum(prints * prints, axis=(1, 2)),
            jnp.sum(chosen * chosen, axis=(1, 2)),
        ]
    )
    totals = lax.psum(totals, EVERY)
    cross, own, refsq = totals[0:2], totals[2:4], totals[4:6]
    scores = D * (cross / squared) / jnp.sqrt((own / squared + 1e-06) * (refsq / squared + 1e-06))
    return prints, scores


def solution(mesh):
    split = Mesh(mesh.devices.reshape(4, 2, 2, 2, 4), EVERY)
    return jax.shard_map(
        body,
        mesh=split,
        in_specs=(
            P(None, TOK, COL),
            P(None, TOK, COL),
            P(None, TOK),
            P(TOK),
            P(COL),
            P(None, TOK, COL),
            P(),
        ),
        out_specs=(P(None, TOK, COL), P()),
        check_vma=False,
    )
```

```python
import functools
import math

import jax
import jax.numpy as jnp
from jax import lax
from jax.experimental import pallas as pl
from jax.experimental.pallas import tpu as pltpu
from jax.sharding import Mesh
from jax.sharding import PartitionSpec as P

D = 4096
TOK = ("tok_0", "tok_1", "tok_2")
COL = ("col_0", "col_1")
EVERY = ("tok_0", "tok_1", "tok_2", "col_0", "col_1")
MESH = pl.DeviceIdType.MESH

SEQS = 2
TOKENS = 1536
HALF = TOKENS // 2
FEATS = 512
BLOCKS = 4
UNITS = SEQS * BLOCKS


def hadamard(order):
    positions = jnp.arange(order, dtype=jnp.int32)
    common_bits = jnp.bitwise_and(positions[:, None], positions[None, :])
    parity = jnp.zeros((order, order), jnp.int32)
    for bit_number in range(max(order.bit_length() - 1, 0)):
        parity = parity + jnp.bitwise_and(jnp.right_shift(common_bits, bit_number), 1)
    return (1 - 2 * (parity % 2)).astype(jnp.float32)


def gather_kernel(
    acts,
    grads,
    row_bits,
    walsh,
    out,
    bits,
    tables,
    a_buf,
    m_buf,
    relay,
    turned,
    part,
    core_in,
    x_half,
    x_full,
    y_in,
    load_sem,
    a_send,
    a_recv,
    m_send,
    m_recv,
    core_send,
    core_recv,
    xh_send,
    xh_recv,
    xf_send,
    xf_recv,
    y_send,
    y_recv,
    bit_load,
    bit_send,
    bit_recv,
):
    x = lax.axis_index("tok_0")
    y_lo = lax.axis_index("tok_1")
    core = lax.axis_index("tok_2")
    y_hi = lax.axis_index("col_0")
    z = lax.axis_index("col_1")
    y = y_hi * 2 + y_lo

    def at_y(value):
        value = lax.rem(value, 4)
        return (x, lax.rem(value, 2), core, lax.div(value, 2), z)

    x_next, x_prev, x_far = lax.rem(x + 1, 4), lax.rem(x + 3, 4), lax.rem(x + 2, 4)
    z_ids = ((x, y_lo, core, y_hi, lax.rem(z + 1, 4)), (x, y_lo, core, y_hi, lax.rem(z + 3, 4)))
    y_ids = (at_y(y + 1), at_y(y + 3))
    x_ids = ((x_next, y_lo, core, y_hi, z), (x_prev, y_lo, core, y_hi, z))
    core_id = (x, y_lo, 1 - core, y_hi, z)
    pair_id = (x, 1 - y_lo, core, y_hi, z)

    loads = []
    for seq in range(SEQS):
        loads.append(pltpu.make_async_copy(acts.at[seq], a_buf.at[seq, 0], load_sem.at[2 * seq]))
        loads.append(pltpu.make_async_copy(grads.at[seq], m_buf.at[seq, 0], load_sem.at[2 * seq + 1]))
    loads.append(pltpu.make_async_copy(row_bits, bits.at[y_lo, x, core], bit_load))
    for copy in loads:
        copy.start()

    barrier = pltpu.get_barrier_semaphore()
    partners = (*z_ids, *y_ids, *x_ids, core_id)
    for partner in partners:
        pl.semaphore_signal(barrier, inc=1, device_id=partner, device_id_type=MESH)
    pl.semaphore_wait(barrier, len(partners))

    def rows_of(half):
        return pl.ds(half * HALF, HALF)

    def remote(src, dst, send, recv, device):
        return pltpu.make_async_remote_copy(
            src_ref=src, dst_ref=dst, send_sem=send, recv_sem=recv, device_id=device, device_id_type=MESH
        )

    def ring_copy(seq, way, half, hop):
        slot = (3, 1)[way] if hop == 0 else 2
        index = (seq * 2 + way) * 3 + (2 if hop else half)
        src = acts.at[seq, rows_of(half)] if hop == 0 else a_buf.at[seq, (3, 1)[way], rows_of(half)]
        return remote(src, a_buf.at[seq, slot, rows_of(half)], a_send.at[index], a_recv.at[index], z_ids[way])

    def swap_copy(seq, way, hop):
        index = (seq * 2 + way) * 2 + hop
        src = relay.at[seq, way] if hop else grads.at[seq, rows_of(way)]
        dst = m_buf.at[seq, 1, rows_of(way)] if hop else relay.at[seq, way]
        return remote(src, dst, m_send.at[index], m_recv.at[index], y_ids[way])

    sent = []

    def start(copy):
        copy.start()
        sent.append(copy)

    def ring_own(seq):
        for step in range(2):
            for way in range(2):
                start(ring_copy(seq, way, (way + step) % 2, 0))

    def ring_pass(seq):
        for way in range(2):
            ring_copy(seq, way, way, 0).wait_recv()
            start(ring_copy(seq, way, way, 1))

    def swap_own(seq):
        for way in range(2):
            start(swap_copy(seq, way, 0))

    def swap_pass(seq):
        for way in range(2):
            swap_copy(seq, way, 0).wait_recv()
            start(swap_copy(seq, way, 1))

    def swap_end(seq):
        for way in range(2):
            swap_copy(seq, way, 1).wait_recv()

    def ring_near(seq, way):
        ring_copy(seq, way, 1 - way, 0).wait_recv()

    def ring_far(seq):
        for way in range(2):
            ring_copy(seq, way, way, 1).wait_recv()

    def bit_copy(index, ref, device):
        return remote(ref, ref, bit_send.at[index], bit_recv.at[index], device)

    def share_bits():
        loads.pop().wait()
        start(bit_copy(0, bits.at[y_lo, x, core], core_id))
        bit_copy(0, bits.at[y_lo, x, core], core_id).wait_recv()
        for way in range(2):
            start(bit_copy(1 + way, bits.at[y_lo, x], x_ids[way]))
        for way in range(2):
            bit_copy(1 + way, bits.at[y_lo, x], x_ids[way]).wait_recv()
        start(bit_copy(3, bits.at[y_lo, x_prev], x_ids[0]))
        bit_copy(3, bits.at[y_lo, x_prev], x_ids[0]).wait_recv()
        start(bit_copy(4, bits.at[y_lo], pair_id))

    def sign_tables():
        bit_copy(4, bits.at[y_lo], pair_id).wait_recv()

        @pl.loop(0, 8)
        def _(i):
            row = bits[lax.rem(lax.div(i, 2), 2), 2 * y_hi + lax.div(i, 4), lax.rem(i, 2)]
            signs = (2 * row - 1).astype(jnp.float32)
            tables[i] = (walsh[...] * signs).astype(jnp.bfloat16)

    core_sign = (1 - 2 * core).astype(jnp.float32)

    def compute(unit, seq, slot):
        block = lax.rem(z + slot, 4)

        @pl.loop(0, 2)
        def _(b):
            columns = pl.ds(pl.multiple_of(b * 256, 256), 256)
            turned[b] = a_buf[seq, slot, :, columns].T

        @pl.loop(0, 4)
        def _(i):
            b = lax.div(i, 2)
            m = lax.rem(i, 2)
            tile = jnp.dot(turned[b], m_buf[seq, m], preferred_element_type=jnp.float32)
            coarse = tile.astype(jnp.bfloat16)
            fine = (tile - coarse.astype(jnp.float32)).astype(jnp.bfloat16)
            table = tables[2 * block + b]
            mixed = jnp.dot(table, coarse, preferred_element_type=jnp.float32)
            mixed += jnp.dot(table, fine, preferred_element_type=jnp.float32)
            columns = pl.ds(pl.multiple_of(lax.rem(m + y_hi, 2) * 512, 512), 512)
            part[unit, b, :, columns] = mixed

        @pl.loop(0, 32)
        def _(i):
            rows = pl.ds(pl.multiple_of(i * 8, 8), 8)
            low = part[unit, 0, rows]
            high = part[unit, 1, rows] * core_sign
            part[unit, 0, rows] = low + high
            part[unit, 1, rows] = low - high

        start(core_copy(unit))

    def core_copy(unit):
        return remote(part.at[unit, 1], core_in.at[unit], core_send.at[unit], core_recv.at[unit], core_id)

    def chunk(unit, x_of):
        return part.at[unit, 0, pl.ds(pl.multiple_of(x_of * 64, 64), 64)]

    def x_half_copy(unit, way):
        rows = pl.ds(pl.multiple_of(x_far * 64 + way * 32, 32), 32)
        index = unit * 2 + way
        return remote(
            part.at[unit, 0, rows], x_half.at[unit, way], xh_send.at[index], xh_recv.at[index], x_ids[way]
        )

    def x_full_copy(unit, way):
        index = unit * 2 + way
        src = chunk(unit, (x_next, x_prev)[way])
        return remote(src, x_full.at[unit, way], xf_send.at[index], xf_recv.at[index], x_ids[way])

    def y_copy(unit):
        rows = pl.ds(pl.multiple_of(x * 64 + (1 - y_lo) * 32, 32), 32)
        return remote(part.at[unit, 0, rows], y_in.at[unit], y_send.at[unit], y_recv.at[unit], pair_id)

    def sum_core(unit):
        core_copy(unit).wait_recv()

        def add(first, rows):
            @pl.loop(0, rows // 8)
            def _(i):
                there = pl.ds(pl.multiple_of(first + i * 8, 8), 8)
                part[unit, 0, there] += core_in[unit, there]

        add(x_far * 64, 64)
        for way in range(2):
            start(x_half_copy(unit, way))
        for other in (x_next, x_prev, x):
            add(other * 64, 64)

    def sum_half(unit):
        for way in range(2):
            x_half_copy(unit, way).wait_recv()
            first = (x_next, x_prev)[way] * 64 + way * 32

            @pl.loop(0, 4)
            def _(i):
                there = pl.ds(pl.multiple_of(first + i * 8, 8), 8)
                part[unit, 0, there] += x_half[unit, way, pl.ds(pl.multiple_of(i * 8, 8), 8)]

            start(x_full_copy(unit, way))

    def sum_full(unit):
        for way in range(2):
            x_full_copy(unit, way).wait_recv()

        @pl.loop(0, 8)
        def _(i):
            there = pl.ds(pl.multiple_of(x * 64 + i * 8, 8), 8)
            here = pl.ds(pl.multiple_of(i * 8, 8), 8)
            part[unit, 0, there] += x_full[unit, 0, here] + x_full[unit, 1, here]

        start(y_copy(unit))

    def finish(unit, seq, slot):
        block = lax.rem(z + slot, 4)
        y_copy(unit).wait_recv()

        @pl.loop(0, 4)
        def _(i):
            here = pl.ds(pl.multiple_of(i * 8, 8), 8)
            there = pl.ds(pl.multiple_of(x * 64 + y_lo * 32 + i * 8, 8), 8)
            out[seq, block, here] = part[unit, 0, there] + y_in[unit, here]

    order = [(seq, slot) for seq in range(SEQS) for slot in (0, 3, 1, 2)]
    run = [functools.partial(compute, unit, *order[unit]) for unit in range(UNITS)]
    end = [functools.partial(finish, unit, *order[unit]) for unit in range(UNITS)]

    ring_own(0)
    swap_own(0)
    share_bits()
    swap_pass(0)
    swap_own(1)
    ring_pass(0)
    ring_own(1)
    for copy in loads:
        copy.wait()
    sign_tables()
    swap_end(0)
    run[0]()
    ring_near(0, 0)
    run[1]()
    sum_core(0)
    ring_near(0, 1)
    run[2]()
    sum_core(1)
    sum_half(0)
    sum_core(2)
    sum_half(1)
    swap_pass(1)
    sum_full(0)
    sum_half(2)
    ring_far(0)
    run[3]()
    sum_core(3)
    sum_full(1)
    end[0]()
    sum_half(3)
    sum_full(2)
    end[1]()
    ring_pass(1)
    swap_end(1)
    run[4]()
    sum_core(4)
    sum_full(3)
    end[2]()
    sum_half(4)
    end[3]()
    sum_full(4)
    ring_near(1, 0)
    run[5]()
    ring_near(1, 1)
    run[6]()
    sum_core(5)
    sum_core(6)
    sum_half(5)
    sum_half(6)
    end[4]()
    sum_full(5)
    sum_full(6)
    ring_far(1)
    run[7]()
    sum_core(7)
    end[5]()
    end[6]()
    sum_half(7)
    sum_full(7)
    end[7]()
    for copy in sent:
        copy.wait_send()


def gathered_products(acts, grads, row_bits, walsh):
    dma = pltpu.SemaphoreType.DMA
    return pl.pallas_call(
        gather_kernel,
        out_shape=jax.ShapeDtypeStruct((SEQS, BLOCKS, 32, 2 * FEATS), jnp.float32),
        in_specs=[
            pl.BlockSpec(memory_space=pl.ANY),
            pl.BlockSpec(memory_space=pl.ANY),
            pl.BlockSpec(memory_space=pl.ANY),
            pl.BlockSpec(memory_space=pltpu.VMEM),
        ],
        out_specs=pl.BlockSpec(memory_space=pltpu.VMEM),
        scratch_shapes=[
            pltpu.VMEM((2, 4, 2, 1, 256), jnp.int32),
            pltpu.VMEM((8, 256, 256), jnp.bfloat16),
            pltpu.VMEM((SEQS, BLOCKS, TOKENS, FEATS), jnp.bfloat16),
            pltpu.VMEM((SEQS, 2, TOKENS, FEATS), jnp.bfloat16),
            pltpu.VMEM((SEQS, 2, HALF, FEATS), jnp.bfloat16),
            pltpu.VMEM((2, 256, TOKENS), jnp.bfloat16),
            pltpu.VMEM((UNITS, 2, 256, 2 * FEATS), jnp.float32),
            pltpu.VMEM((UNITS, 256, 2 * FEATS), jnp.float32),
            pltpu.VMEM((UNITS, 2, 32, 2 * FEATS), jnp.float32),
            pltpu.VMEM((UNITS, 2, 64, 2 * FEATS), jnp.float32),
            pltpu.VMEM((UNITS, 32, 2 * FEATS), jnp.float32),
            dma((4,)),
            dma((12,)),
            dma((12,)),
            dma((8,)),
            dma((8,)),
            dma((UNITS,)),
            dma((UNITS,)),
            dma((2 * UNITS,)),
            dma((2 * UNITS,)),
            dma((2 * UNITS,)),
            dma((2 * UNITS,)),
            dma((UNITS,)),
            dma((UNITS,)),
            dma,
            dma((5,)),
            dma((5,)),
        ],
        compiler_params=pltpu.CompilerParams(
            collective_id=0, has_side_effects=True, vmem_limit_bytes=67043328
        ),
    )(acts, grads, row_bits, walsh)


def mix_kernel(
    sums,
    chosen,
    walsh,
    out,
    totals,
    work,
    got,
    ready,
    land,
    mine,
    theirs,
    late,
    late_in,
    col_send,
    col_recv,
    grp_send,
    grp_recv,
    red_send,
    red_recv,
    late_send,
    late_recv,
):
    x = lax.axis_index("tok_0")
    y_lo = lax.axis_index("tok_1")
    core = lax.axis_index("tok_2")
    y_hi = lax.axis_index("col_0")
    z = lax.axis_index("col_1")
    col_me = y_hi * 4 + z
    grp_me = x * 8 + y_lo * 4 + z

    def col_peer(j):
        there_y = lax.rem(y_hi + lax.div(j, 4), 2)
        there_z = lax.rem(z + j, 4)
        return there_y * 4 + there_z, (x, y_lo, core, there_y, there_z)

    def grp_peer(j):
        there_x = lax.rem(x + lax.div(j, 8), 4)
        there_y = lax.rem(y_lo + lax.div(j, 4), 2)
        there_z = lax.rem(z + j, 4)
        return there_x * 8 + there_y * 4 + there_z, (there_x, there_y, core, y_hi, there_z)

    core_id = (x, y_lo, 1 - core, y_hi, z)
    far_id = (x, y_lo, core, 1 - y_hi, z)

    barrier = pltpu.get_barrier_semaphore()

    @pl.loop(1, 8)
    def _(j):
        pl.semaphore_signal(barrier, inc=1, device_id=col_peer(j)[1], device_id_type=MESH)

    @pl.loop(1, 32)
    def _(j):
        pl.semaphore_signal(barrier, inc=1, device_id=grp_peer(j)[1], device_id_type=MESH)

    pl.semaphore_signal(barrier, inc=1, device_id=core_id, device_id_type=MESH)

    def remote(src, dst, send, recv, device):
        return pltpu.make_async_remote_copy(
            src_ref=src, dst_ref=dst, send_sem=send, recv_sem=recv, device_id=device, device_id_type=MESH
        )

    def piece(peer):
        return pl.ds(pl.multiple_of(peer * 32, 32), 32)

    def col_copy(seq, j):
        peer, device = col_peer(j)
        return remote(
            work.at[seq, piece(peer)], got.at[seq, col_me], col_send.at[seq, j], col_recv.at[seq, j], device
        )

    def grp_copy(seq, j):
        peer, device = grp_peer(j)
        return remote(
            ready.at[seq, peer], land.at[seq, grp_me], grp_send.at[seq, j], grp_recv.at[seq, j], device
        )

    def red_copy(j):
        return remote(mine, theirs.at[grp_me], red_send.at[j], red_recv.at[j], grp_peer(j)[1])

    def late_copy(step):
        return remote(
            late.at[step], late_in.at[step], late_send.at[step], late_recv.at[step], (far_id, core_id)[step]
        )

    def pair(low, high):
        return low + high, low - high

    def four(values):
        a, b = pair(values[0], values[2])
        c, d = pair(values[1], values[3])
        first, second = pair(a, c)
        third, fourth = pair(b, d)
        return first, second, third, fourth

    def mix_local(seq):
        @pl.loop(0, 4)
        def _(q):
            rows = pl.ds(pl.multiple_of(q * 8, 8), 8)
            for half in range(2):
                columns = slice(half * 256, half * 256 + 256)
                upper = slice(512 + half * 256, 768 + half * 256)
                left = four([sums[seq, a, rows, columns] for a in range(4)])
                right = four([sums[seq, a, rows, upper] for a in range(4)])
                for a in range(4):
                    low, high = pair(left[a], right[a])
                    work[seq, pl.ds(pl.multiple_of(q * 32 + a * 8, 8), 8), columns] = low
                    work[seq, pl.ds(pl.multiple_of(128 + q * 32 + a * 8, 8), 8), columns] = high

        values = work[seq]
        coarse = values.astype(jnp.bfloat16)
        fine = (values - coarse.astype(jnp.float32)).astype(jnp.bfloat16)
        mixed = jnp.dot(coarse, walsh[...], preferred_element_type=jnp.float32)
        mixed += jnp.dot(fine, walsh[...], preferred_element_type=jnp.float32)
        work[seq] = mixed * (1.0 / D)

    def mix_cols(seq):
        @pl.loop(0, 4)
        def _(o):
            for part in range(2):
                columns = slice(part * 256, part * 256 + 256)
                rows = pl.ds(pl.multiple_of(o * 8, 8), 8)
                left = four([got[seq, src, rows, columns] for src in range(4)])
                right = four([got[seq, 4 + src, rows, columns] for src in range(4)])
                for c in range(4):
                    low, high = pair(left[c], right[c])
                    ready[seq, o * 4 + c, :, columns] = low
                    ready[seq, 16 + o * 4 + c, :, columns] = high

    for seq in range(SEQS):
        mix_local(seq)
        if seq == 0:
            pl.semaphore_wait(barrier, 39)

        @pl.loop(1, 8)
        def _(j):
            col_copy(seq, j).start()

        got[seq, col_me] = work[seq, piece(col_me)]

    for seq in range(SEQS):

        @pl.loop(1, 8)
        def _(j):
            col_copy(seq, j).wait_recv()

        mix_cols(seq)

        @pl.loop(1, 32)
        def _(j):
            grp_copy(seq, j).start()

        land[seq, grp_me] = ready[seq, grp_me]

    mine[...] = jnp.zeros((8, 128), jnp.float32)
    for seq in range(SEQS):

        @pl.loop(1, 32)
        def _(j):
            grp_copy(seq, j).wait_recv()

        def add(i, carry):
            rows = pl.ds(pl.multiple_of(i * 8, 8), 8)
            value = land[seq, i]
            other = chosen[seq, rows]
            out[seq, rows] = value
            terms = (value * other, value * value, other * other)
            return tuple(total + term for total, term in zip(carry, terms))

        start = tuple(jnp.zeros((8, 512), jnp.float32) for _ in range(3))
        for kind, total in enumerate(lax.fori_loop(0, 32, add, start)):
            total = total[:, 0:128] + total[:, 128:256] + total[:, 256:384] + total[:, 384:512]
            mine[2 * kind + seq : 2 * kind + seq + 1, :] = jnp.sum(total, axis=0, keepdims=True)

    @pl.loop(1, 32)
    def _(j):
        red_copy(j).start()

    theirs[grp_me] = mine[...]

    @pl.loop(1, 32)
    def _(j):
        red_copy(j).wait_recv()

    late[0] = lax.fori_loop(0, 32, lambda i, total: total + theirs[i], jnp.zeros((8, 128), jnp.float32))
    for step in range(2):
        late_copy(step).start()
        late_copy(step).wait_recv()
        both = late[step] + late_in[step]
        if step == 0:
            late[1] = both
    totals[...] = jnp.broadcast_to(jnp.sum(both, axis=1, keepdims=True), (8, 128))

    for seq in range(SEQS):

        @pl.loop(1, 8)
        def _(j):
            col_copy(seq, j).wait_send()

        @pl.loop(1, 32)
        def _(j):
            grp_copy(seq, j).wait_send()

    @pl.loop(1, 32)
    def _(j):
        red_copy(j).wait_send()

    for step in range(2):
        late_copy(step).wait_send()


def mixed_prints(sums, chosen, walsh):
    dma = pltpu.SemaphoreType.DMA
    vmem = pl.BlockSpec(memory_space=pltpu.VMEM)
    return pl.pallas_call(
        mix_kernel,
        out_shape=(
            jax.ShapeDtypeStruct((SEQS, 256, 512), jnp.float32),
            jax.ShapeDtypeStruct((8, 128), jnp.float32),
        ),
        in_specs=[vmem, vmem, vmem],
        out_specs=(vmem, vmem),
        scratch_shapes=[
            pltpu.VMEM((SEQS, 256, 512), jnp.float32),
            pltpu.VMEM((SEQS, 8, 32, 512), jnp.float32),
            pltpu.VMEM((SEQS, 32, 8, 512), jnp.float32),
            pltpu.VMEM((SEQS, 32, 8, 512), jnp.float32),
            pltpu.VMEM((8, 128), jnp.float32),
            pltpu.VMEM((32, 8, 128), jnp.float32),
            pltpu.VMEM((2, 8, 128), jnp.float32),
            pltpu.VMEM((2, 8, 128), jnp.float32),
            dma((SEQS, 8)),
            dma((SEQS, 8)),
            dma((SEQS, 32)),
            dma((SEQS, 32)),
            dma((32,)),
            dma((32,)),
            dma((2,)),
            dma((2,)),
        ],
        compiler_params=pltpu.CompilerParams(
            collective_id=1, has_side_effects=True, vmem_limit_bytes=32 * 1024 * 1024
        ),
    )(sums, chosen, walsh)


def body(activations, out_grads, token_mask, row_signs, col_signs, bank, bank_index):
    squared = float(D) * float(D)
    col_pm = (2 * col_signs - 1).astype(jnp.bfloat16)
    grads = out_grads * token_mask[:, :, None].astype(jnp.bfloat16) * col_pm[None, None, :]
    sums = gathered_products(activations, grads, row_signs.reshape(1, 256), hadamard(256))
    chosen = jnp.stack(
        [lax.dynamic_index_in_dim(bank, bank_index[seq], 0, keepdims=False) for seq in range(SEQS)]
    )
    prints, totals = mixed_prints(sums, chosen, hadamard(512).astype(jnp.bfloat16))
    cross, own, refsq = totals[0:2, 0], totals[2:4, 0], totals[4:6, 0]
    scores = D * (cross / squared) / jnp.sqrt((own / squared + 1e-06) * (refsq / squared + 1e-06))
    return prints, scores


def solution(mesh):
    split = Mesh(mesh.devices.reshape(4, 2, 2, 2, 4), EVERY)
    return jax.shard_map(
        body,
        mesh=split,
        in_specs=(
            P(None, TOK, COL),
            P(None, TOK, COL),
            P(None, TOK),
            P(TOK),
            P(COL),
            P(None, TOK, COL),
            P(),
        ),
        out_specs=(P(None, TOK, COL), P()),
        check_vma=False,
    )
```

```python
import functools
import math

import jax
import jax.numpy as jnp
from jax import lax
from jax.experimental import pallas as pl
from jax.experimental.pallas import tpu as pltpu
from jax.sharding import Mesh
from jax.sharding import PartitionSpec as P

D = 4096
TOK = ("tok_0", "tok_1", "tok_2")
COL = ("col_0", "col_1")
EVERY = ("tok_0", "tok_1", "tok_2", "col_0", "col_1")
MESH = pl.DeviceIdType.MESH

SEQS = 2
TOKENS = 1536
HALF = TOKENS // 2
FEATS = 512
BLOCKS = 4
UNITS = SEQS * BLOCKS * 2

ORDER = (
    ('run', 0, 0, 0),
    ('run', 1, 0, 0),
    ('core', 0, 0, 0),
    ('core', 1, 0, 0),
    ('half', 0, 0, 0),
    ('half', 1, 0, 0),
    ('spass', 0),
    ('rpass', 0),
    ('full', 0, 0, 0),
    ('full', 1, 0, 0),
    ('run', 0, 3, 0),
    ('run', 0, 0, 1),
    ('core', 0, 3, 0),
    ('run', 0, 3, 1),
    ('core', 0, 0, 1),
    ('run', 0, 1, 0),
    ('half', 0, 3, 0),
    ('core', 0, 3, 1),
    ('run', 0, 1, 1),
    ('half', 0, 0, 1),
    ('core', 0, 1, 0),
    ('core', 0, 1, 1),
    ('full', 0, 3, 0),
    ('half', 0, 3, 1),
    ('run', 0, 2, 0),
    ('spass', 1),
    ('full', 0, 0, 1),
    ('run', 0, 2, 1),
    ('half', 0, 1, 0),
    ('core', 0, 2, 0),
    ('half', 0, 1, 1),
    ('end', 0, 0, 0),
    ('end', 1, 0, 0),
    ('end', 0, 3, 0),
    ('core', 0, 2, 1),
    ('full', 0, 3, 1),
    ('full', 0, 1, 0),
    ('half', 0, 2, 0),
    ('full', 0, 1, 1),
    ('half', 0, 2, 1),
    ('rpass', 1),
    ('full', 0, 2, 0),
    ('full', 0, 2, 1),
    ('run', 1, 0, 1),
    ('end', 0, 0, 1),
    ('end', 0, 3, 1),
    ('core', 1, 0, 1),
    ('end', 0, 1, 0),
    ('end', 0, 1, 1),
    ('end', 0, 2, 0),
    ('half', 1, 0, 1),
    ('end', 0, 2, 1),
    ('run', 1, 3, 0),
    ('full', 1, 0, 1),
    ('run', 1, 3, 1),
    ('core', 1, 3, 0),
    ('run', 1, 1, 0),
    ('core', 1, 3, 1),
    ('run', 1, 1, 1),
    ('half', 1, 3, 0),
    ('core', 1, 1, 0),
    ('end', 1, 0, 1),
    ('half', 1, 3, 1),
    ('core', 1, 1, 1),
    ('full', 1, 3, 0),
    ('half', 1, 1, 0),
    ('run', 1, 2, 0),
    ('run', 1, 2, 1),
    ('full', 1, 3, 1),
    ('half', 1, 1, 1),
    ('core', 1, 2, 0),
    ('end', 1, 3, 0),
    ('core', 1, 2, 1),
    ('full', 1, 1, 0),
    ('end', 1, 3, 1),
    ('full', 1, 1, 1),
    ('end', 1, 1, 0),
    ('half', 1, 2, 0),
    ('half', 1, 2, 1),
    ('end', 1, 1, 1),
    ('full', 1, 2, 0),
    ('full', 1, 2, 1),
    ('end', 1, 2, 0),
    ('end', 1, 2, 1),
)


def hadamard_rows(first, rows, order):
    down = lax.broadcasted_iota(jnp.int32, (rows, order), 0) + first
    common_bits = jnp.bitwise_and(down, lax.broadcasted_iota(jnp.int32, (rows, order), 1))
    for shift in (8, 4, 2, 1):
        common_bits = jnp.bitwise_xor(common_bits, jnp.right_shift(common_bits, shift))
    return (1 - 2 * jnp.bitwise_and(common_bits, 1)).astype(jnp.float32)


def gather_kernel(
    acts,
    grads,
    row_bits,
    col_bits,
    mask,
    out,
    bits,
    walsh,
    tables,
    a_buf,
    m_buf,
    relay,
    part,
    core_in,
    x_half,
    x_full,
    y_in,
    load_sem,
    a_send,
    a_recv,
    m_send,
    m_recv,
    core_send,
    core_recv,
    xh_send,
    xh_recv,
    xf_send,
    xf_recv,
    y_send,
    y_recv,
    bit_load,
    bit_send,
    bit_recv,
):
    x = lax.axis_index("tok_0")
    y_lo = lax.axis_index("tok_1")
    core = lax.axis_index("tok_2")
    y_hi = lax.axis_index("col_0")
    z = lax.axis_index("col_1")
    y = y_hi * 2 + y_lo

    def at_y(value):
        value = lax.rem(value, 4)
        return (x, lax.rem(value, 2), core, lax.div(value, 2), z)

    x_next, x_prev, x_far = lax.rem(x + 1, 4), lax.rem(x + 3, 4), lax.rem(x + 2, 4)
    z_ids = ((x, y_lo, core, y_hi, lax.rem(z + 1, 4)), (x, y_lo, core, y_hi, lax.rem(z + 3, 4)))
    y_ids = (at_y(y + 1), at_y(y + 3))
    x_ids = ((x_next, y_lo, core, y_hi, z), (x_prev, y_lo, core, y_hi, z))
    core_id = (x, y_lo, 1 - core, y_hi, z)
    pair_id = (x, 1 - y_lo, core, y_hi, z)

    bit_own = pltpu.make_async_copy(row_bits, bits.at[core, x, y_lo], bit_load)
    m_own = [pltpu.make_async_copy(grads.at[seq], m_buf.at[seq, 0], load_sem.at[seq]) for seq in range(SEQS)]
    a_own = [pltpu.make_async_copy(acts.at[seq], a_buf.at[seq, 0], load_sem.at[2 + seq]) for seq in range(SEQS)]
    for copy in (bit_own, *m_own, *a_own):
        copy.start()

    barrier = pltpu.get_barrier_semaphore()
    partners = (*z_ids, *y_ids, *x_ids, core_id)
    for partner in partners:
        pl.semaphore_signal(barrier, inc=1, device_id=partner, device_id_type=MESH)
    pl.semaphore_wait(barrier, len(partners))

    def rows_of(half):
        return pl.ds(half * HALF, HALF)

    def remote(src, dst, send, recv, device):
        return pltpu.make_async_remote_copy(
            src_ref=src, dst_ref=dst, send_sem=send, recv_sem=recv, device_id=device, device_id_type=MESH
        )

    def ring_copy(seq, way, half, hop):
        slot = (3, 1)[way] if hop == 0 else 2
        index = (seq * 2 + way) * 3 + (2 if hop else half)
        src = acts.at[seq, rows_of(half)] if hop == 0 else a_buf.at[seq, (3, 1)[way], rows_of(half)]
        return remote(src, a_buf.at[seq, slot, rows_of(half)], a_send.at[index], a_recv.at[index], z_ids[way])

    def swap_copy(seq, way, hop):
        index = (seq * 2 + way) * 2 + hop
        src = relay.at[seq, way] if hop else m_buf.at[seq, 0, rows_of(way)]
        dst = m_buf.at[seq, 1, rows_of(way)] if hop else relay.at[seq, way]
        return remote(src, dst, m_send.at[index], m_recv.at[index], y_ids[way])

    sent = []

    def start(copy):
        copy.start()
        sent.append(copy)

    def ring_own(seq):
        for step in range(2):
            for way in range(2):
                start(ring_copy(seq, way, (way + step) % 2, 0))

    def ring_pass(seq):
        for way in range(2):
            ring_copy(seq, way, way, 0).wait_recv()
            start(ring_copy(seq, way, way, 1))

    def swap_own(seq):
        for way in range(2):
            start(swap_copy(seq, way, 0))

    def swap_pass(seq):
        for way in range(2):
            swap_copy(seq, way, 0).wait_recv()
            start(swap_copy(seq, way, 1))

    def swap_end(seq):
        for way in range(2):
            swap_copy(seq, way, 1).wait_recv()

    def ring_near(seq, way):
        ring_copy(seq, way, 1 - way, 0).wait_recv()

    def ring_far(seq):
        for way in range(2):
            ring_copy(seq, way, way, 1).wait_recv()

    def bit_copy(index, ref, device):
        return remote(ref, ref, bit_send.at[index], bit_recv.at[index], device)

    def share_bits():
        for way in range(2):
            start(bit_copy(1 + way, bits.at[core, x], x_ids[way]))
        for way in range(2):
            bit_copy(1 + way, bits.at[core, x], x_ids[way]).wait_recv()
        start(bit_copy(3, bits.at[core, x_prev], x_ids[0]))
        bit_copy(3, bits.at[core, x_prev], x_ids[0]).wait_recv()
        start(bit_copy(4, bits.at[core], core_id))

    def sign_tables():
        bit_copy(4, bits.at[core], core_id).wait_recv()

        @pl.loop(0, 8)
        def _(i):
            row = bits[lax.rem(i, 2), 2 * y_hi + lax.div(i, 4), lax.rem(lax.div(i, 2), 2)]
            signs = (2 * row - 1).astype(jnp.float32)
            tables[i] = (walsh[...] * signs).astype(jnp.bfloat16)

    def column_signs(seq):
        signs = (2 * col_bits[...] - 1).astype(jnp.float32).astype(jnp.bfloat16)

        @pl.loop(0, TOKENS // 32)
        def _(i):
            rows = pl.ds(pl.multiple_of(i * 32, 32), 32)
            m_buf[seq, 0, rows] = m_buf[seq, 0, rows] * signs

    core_sign = (1 - 2 * core).astype(jnp.float32)

    def compute(unit, seq, slot, m):
        block = lax.rem(z + slot, 4)
        counted = mask[seq].astype(jnp.float32).astype(jnp.bfloat16)

        @pl.loop(0, 2)
        def _(b):
            columns = pl.ds(pl.multiple_of(b * 256, 256), 256)
            rows_first = a_buf[seq, slot, :, columns].T * counted
            tile = jnp.dot(rows_first, m_buf[seq, m], preferred_element_type=jnp.float32)
            coarse = tile.astype(jnp.bfloat16)
            fine = (tile - coarse.astype(jnp.float32)).astype(jnp.bfloat16)
            table = tables[2 * block + b]
            mixed = jnp.dot(table, coarse, preferred_element_type=jnp.float32)
            mixed += jnp.dot(table, fine, preferred_element_type=jnp.float32)
            part[unit, b] = mixed

        @pl.loop(0, 16)
        def _(i):
            rows = pl.ds(pl.multiple_of(i * 16, 16), 16)
            low = part[unit, 0, rows]
            high = part[unit, 1, rows] * core_sign
            part[unit, 0, rows] = low + high
            part[unit, 1, rows] = low - high

        start(core_copy(unit))

    def core_copy(unit):
        return remote(part.at[unit, 1], core_in.at[unit], core_send.at[unit], core_recv.at[unit], core_id)

    def chunk(unit, x_of):
        return part.at[unit, 0, pl.ds(pl.multiple_of(x_of * 64, 64), 64)]

    def x_half_copy(unit, way):
        rows = pl.ds(pl.multiple_of(x_far * 64 + way * 32, 32), 32)
        index = unit * 2 + way
        return remote(
            part.at[unit, 0, rows], x_half.at[unit, way], xh_send.at[index], xh_recv.at[index], x_ids[way]
        )

    def x_full_copy(unit, way):
        index = unit * 2 + way
        src = chunk(unit, (x_next, x_prev)[way])
        return remote(src, x_full.at[unit, way], xf_send.at[index], xf_recv.at[index], x_ids[way])

    def y_copy(unit):
        rows = pl.ds(pl.multiple_of(x * 64 + (1 - y_lo) * 32, 32), 32)
        return remote(part.at[unit, 0, rows], y_in.at[unit], y_send.at[unit], y_recv.at[unit], pair_id)

    def sum_core(unit):
        core_copy(unit).wait_recv()

        def add(first, rows):
            @pl.loop(0, rows // 8)
            def _(i):
                there = pl.ds(pl.multiple_of(first + i * 8, 8), 8)
                part[unit, 0, there] += core_in[unit, there]

        add(x_far * 64, 64)
        for way in range(2):
            start(x_half_copy(unit, way))
        for other in (x_next, x_prev, x):
            add(other * 64, 64)

    def sum_half(unit):
        for way in range(2):
            x_half_copy(unit, way).wait_recv()
            first = (x_next, x_prev)[way] * 64 + way * 32

            @pl.loop(0, 4)
            def _(i):
                there = pl.ds(pl.multiple_of(first + i * 8, 8), 8)
                part[unit, 0, there] += x_half[unit, way, pl.ds(pl.multiple_of(i * 8, 8), 8)]

            start(x_full_copy(unit, way))

    def sum_full(unit):
        for way in range(2):
            x_full_copy(unit, way).wait_recv()

        @pl.loop(0, 8)
        def _(i):
            there = pl.ds(pl.multiple_of(x * 64 + i * 8, 8), 8)
            here = pl.ds(pl.multiple_of(i * 8, 8), 8)
            part[unit, 0, there] += x_full[unit, 0, here] + x_full[unit, 1, here]

        start(y_copy(unit))

    def finish(unit, seq, slot, m):
        block = lax.rem(z + slot, 4)
        columns = pl.ds(pl.multiple_of(lax.rem(m + y_hi, 2) * FEATS, FEATS), FEATS)
        y_copy(unit).wait_recv()

        @pl.loop(0, 4)
        def _(i):
            here = pl.ds(pl.multiple_of(i * 8, 8), 8)
            there = pl.ds(pl.multiple_of(x * 64 + y_lo * 32 + i * 8, 8), 8)
            out[seq, block, here, columns] = part[unit, 0, there] + y_in[unit, here]

    ring_own(0)
    walsh[...] = hadamard_rows(0, 256, 256)
    bit_own.wait()
    start(bit_copy(0, bits.at[core, x, y_lo], pair_id))
    m_own[0].wait()
    column_signs(0)
    swap_own(0)
    bit_copy(0, bits.at[core, x, y_lo], pair_id).wait_recv()
    share_bits()
    m_own[1].wait()
    column_signs(1)
    for copy in a_own:
        copy.wait()
    sign_tables()

    here = {("a", 0, 0), ("a", 1, 0), ("m", 0, 0), ("m", 1, 0)}

    def once(key, wait):
        if key not in here:
            here.add(key)
            wait()

    for step, *rest in ORDER:
        if step == "spass":
            swap_pass(rest[0])
            if rest[0] == 0:
                swap_own(1)
            continue
        if step == "rpass":
            ring_pass(rest[0])
            if rest[0] == 0:
                ring_own(1)
            continue
        seq, slot, m = rest
        unit = (seq * BLOCKS + slot) * 2 + m
        if step == "run":
            if slot == 2:
                once(("a", seq, 2), lambda seq=seq: ring_far(seq))
            else:
                once(("a", seq, slot), lambda seq=seq, slot=slot: ring_near(seq, 0 if slot == 3 else 1))
            once(("m", seq, m), lambda seq=seq: swap_end(seq))
            compute(unit, seq, slot, m)
        elif step == "core":
            sum_core(unit)
        elif step == "half":
            sum_half(unit)
        elif step == "full":
            sum_full(unit)
        else:
            finish(unit, seq, slot, m)
    for copy in sent:
        copy.wait_send()


def gathered_products(acts, grads, row_bits, col_bits, mask):
    dma = pltpu.SemaphoreType.DMA
    return pl.pallas_call(
        gather_kernel,
        out_shape=jax.ShapeDtypeStruct((SEQS, BLOCKS, 32, 2 * FEATS), jnp.float32),
        in_specs=[
            pl.BlockSpec(memory_space=pl.ANY),
            pl.BlockSpec(memory_space=pl.ANY),
            pl.BlockSpec(memory_space=pl.ANY),
            pl.BlockSpec(memory_space=pltpu.VMEM),
            pl.BlockSpec(memory_space=pltpu.VMEM),
        ],
        out_specs=pl.BlockSpec(memory_space=pltpu.VMEM),
        scratch_shapes=[
            pltpu.VMEM((2, 4, 2, 1, 256), jnp.int32),
            pltpu.VMEM((256, 256), jnp.float32),
            pltpu.VMEM((8, 256, 256), jnp.bfloat16),
            pltpu.VMEM((SEQS, BLOCKS, TOKENS, FEATS), jnp.bfloat16),
            pltpu.VMEM((SEQS, 2, TOKENS, FEATS), jnp.bfloat16),
            pltpu.VMEM((SEQS, 2, HALF, FEATS), jnp.bfloat16),
            pltpu.VMEM((UNITS, 2, 256, FEATS), jnp.float32),
            pltpu.VMEM((UNITS, 256, FEATS), jnp.float32),
            pltpu.VMEM((UNITS, 2, 32, FEATS), jnp.float32),
            pltpu.VMEM((UNITS, 2, 64, FEATS), jnp.float32),
            pltpu.VMEM((UNITS, 32, FEATS), jnp.float32),
            dma((4,)),
            dma((12,)),
            dma((12,)),
            dma((8,)),
            dma((8,)),
            dma((UNITS,)),
            dma((UNITS,)),
            dma((2 * UNITS,)),
            dma((2 * UNITS,)),
            dma((2 * UNITS,)),
            dma((2 * UNITS,)),
            dma((UNITS,)),
            dma((UNITS,)),
            dma,
            dma((5,)),
            dma((5,)),
        ],
        compiler_params=pltpu.CompilerParams(
            collective_id=0, has_side_effects=True, vmem_limit_bytes=67043328
        ),
    )(acts, grads, row_bits, col_bits, mask)


def mix_kernel(
    sums,
    chosen_0,
    chosen_1,
    out,
    totals,
    walsh,
    work,
    got,
    ready,
    land,
    mine,
    theirs,
    late,
    late_in,
    col_send,
    col_recv,
    grp_send,
    grp_recv,
    red_send,
    red_recv,
    late_send,
    late_recv,
):
    x = lax.axis_index("tok_0")
    y_lo = lax.axis_index("tok_1")
    core = lax.axis_index("tok_2")
    y_hi = lax.axis_index("col_0")
    z = lax.axis_index("col_1")
    col_me = y_hi * 4 + z
    grp_me = x * 8 + y_lo * 4 + z

    def col_peer(j):
        there_y = lax.rem(y_hi + lax.div(j, 4), 2)
        there_z = lax.rem(z + j, 4)
        return there_y * 4 + there_z, (x, y_lo, core, there_y, there_z)

    def grp_peer(j):
        there_x = lax.rem(x + lax.div(j, 8), 4)
        there_y = lax.rem(y_lo + lax.div(j, 4), 2)
        there_z = lax.rem(z + j, 4)
        return there_x * 8 + there_y * 4 + there_z, (there_x, there_y, core, y_hi, there_z)

    core_id = (x, y_lo, 1 - core, y_hi, z)
    far_id = (x, y_lo, core, 1 - y_hi, z)

    barrier = pltpu.get_barrier_semaphore()

    @pl.loop(1, 8)
    def _(j):
        pl.semaphore_signal(barrier, inc=1, device_id=col_peer(j)[1], device_id_type=MESH)

    @pl.loop(1, 32)
    def _(j):
        pl.semaphore_signal(barrier, inc=1, device_id=grp_peer(j)[1], device_id_type=MESH)

    pl.semaphore_signal(barrier, inc=1, device_id=core_id, device_id_type=MESH)

    @pl.loop(0, 8)
    def _(i):
        rows = pl.ds(pl.multiple_of(i * 64, 64), 64)
        walsh[rows] = hadamard_rows(i * 64, 64, 512).astype(jnp.bfloat16)

    def remote(src, dst, send, recv, device):
        return pltpu.make_async_remote_copy(
            src_ref=src, dst_ref=dst, send_sem=send, recv_sem=recv, device_id=device, device_id_type=MESH
        )

    def piece(peer):
        return pl.ds(pl.multiple_of(peer * 32, 32), 32)

    def col_copy(seq, j):
        peer, device = col_peer(j)
        return remote(
            work.at[seq, piece(peer)], got.at[seq, col_me], col_send.at[seq, j], col_recv.at[seq, j], device
        )

    def grp_copy(seq, j):
        peer, device = grp_peer(j)
        return remote(
            ready.at[seq, peer], land.at[seq, grp_me], grp_send.at[seq, j], grp_recv.at[seq, j], device
        )

    def red_copy(j):
        return remote(mine, theirs.at[grp_me], red_send.at[j], red_recv.at[j], grp_peer(j)[1])

    def late_copy(step):
        return remote(
            late.at[step], late_in.at[step], late_send.at[step], late_recv.at[step], (far_id, core_id)[step]
        )

    def pair(low, high):
        return low + high, low - high

    def four(values):
        a, b = pair(values[0], values[2])
        c, d = pair(values[1], values[3])
        first, second = pair(a, c)
        third, fourth = pair(b, d)
        return first, second, third, fourth

    def mix_local(seq):
        @pl.loop(0, 4)
        def _(q):
            rows = pl.ds(pl.multiple_of(q * 8, 8), 8)
            for half in range(2):
                columns = slice(half * 256, half * 256 + 256)
                upper = slice(512 + half * 256, 768 + half * 256)
                left = four([sums[seq, a, rows, columns] for a in range(4)])
                right = four([sums[seq, a, rows, upper] for a in range(4)])
                for a in range(4):
                    low, high = pair(left[a], right[a])
                    work[seq, pl.ds(pl.multiple_of(q * 32 + a * 8, 8), 8), columns] = low
                    work[seq, pl.ds(pl.multiple_of(128 + q * 32 + a * 8, 8), 8), columns] = high

        values = work[seq]
        coarse = values.astype(jnp.bfloat16)
        fine = (values - coarse.astype(jnp.float32)).astype(jnp.bfloat16)
        mixed = jnp.dot(coarse, walsh[...], preferred_element_type=jnp.float32)
        mixed += jnp.dot(fine, walsh[...], preferred_element_type=jnp.float32)
        work[seq] = mixed * (1.0 / D)

    def mix_cols(seq):
        @pl.loop(0, 4)
        def _(o):
            for part in range(2):
                columns = slice(part * 256, part * 256 + 256)
                rows = pl.ds(pl.multiple_of(o * 8, 8), 8)
                left = four([got[seq, src, rows, columns] for src in range(4)])
                right = four([got[seq, 4 + src, rows, columns] for src in range(4)])
                for c in range(4):
                    low, high = pair(left[c], right[c])
                    ready[seq, o * 4 + c, :, columns] = low
                    ready[seq, 16 + o * 4 + c, :, columns] = high

    for seq in range(SEQS):
        mix_local(seq)
        if seq == 0:
            pl.semaphore_wait(barrier, 39)

        @pl.loop(1, 8)
        def _(j):
            col_copy(seq, j).start()

        got[seq, col_me] = work[seq, piece(col_me)]

    for seq in range(SEQS):

        @pl.loop(1, 8)
        def _(j):
            col_copy(seq, j).wait_recv()

        mix_cols(seq)

        @pl.loop(1, 32)
        def _(j):
            grp_copy(seq, j).start()

        land[seq, grp_me] = ready[seq, grp_me]

    mine[...] = jnp.zeros((8, 128), jnp.float32)
    for seq in range(SEQS):

        @pl.loop(1, 32)
        def _(j):
            grp_copy(seq, j).wait_recv()

        def add(i, carry):
            rows = pl.ds(pl.multiple_of(i * 8, 8), 8)
            value = land[seq, i]
            other = (chosen_0, chosen_1)[seq][rows]
            out[seq, rows] = value
            terms = (value * other, value * value, other * other)
            return tuple(total + term for total, term in zip(carry, terms))

        start = tuple(jnp.zeros((8, 512), jnp.float32) for _ in range(3))
        for kind, total in enumerate(lax.fori_loop(0, 32, add, start)):
            total = total[:, 0:128] + total[:, 128:256] + total[:, 256:384] + total[:, 384:512]
            mine[2 * kind + seq : 2 * kind + seq + 1, :] = jnp.sum(total, axis=0, keepdims=True)

    @pl.loop(1, 32)
    def _(j):
        red_copy(j).start()

    theirs[grp_me] = mine[...]

    @pl.loop(1, 32)
    def _(j):
        red_copy(j).wait_recv()

    late[0] = lax.fori_loop(0, 32, lambda i, total: total + theirs[i], jnp.zeros((8, 128), jnp.float32))
    for step in range(2):
        late_copy(step).start()
        late_copy(step).wait_recv()
        both = late[step] + late_in[step]
        if step == 0:
            late[1] = both
    totals[...] = jnp.broadcast_to(jnp.sum(both, axis=1, keepdims=True), (8, 128))

    for seq in range(SEQS):

        @pl.loop(1, 8)
        def _(j):
            col_copy(seq, j).wait_send()

        @pl.loop(1, 32)
        def _(j):
            grp_copy(seq, j).wait_send()

    @pl.loop(1, 32)
    def _(j):
        red_copy(j).wait_send()

    for step in range(2):
        late_copy(step).wait_send()


def mixed_prints(sums, chosen_0, chosen_1):
    dma = pltpu.SemaphoreType.DMA
    vmem = pl.BlockSpec(memory_space=pltpu.VMEM)
    return pl.pallas_call(
        mix_kernel,
        out_shape=(
            jax.ShapeDtypeStruct((SEQS, 256, 512), jnp.float32),
            jax.ShapeDtypeStruct((8, 128), jnp.float32),
        ),
        in_specs=[vmem, vmem, vmem],
        out_specs=(vmem, vmem),
        scratch_shapes=[
            pltpu.VMEM((512, 512), jnp.bfloat16),
            pltpu.VMEM((SEQS, 256, 512), jnp.float32),
            pltpu.VMEM((SEQS, 8, 32, 512), jnp.float32),
            pltpu.VMEM((SEQS, 32, 8, 512), jnp.float32),
            pltpu.VMEM((SEQS, 32, 8, 512), jnp.float32),
            pltpu.VMEM((8, 128), jnp.float32),
            pltpu.VMEM((32, 8, 128), jnp.float32),
            pltpu.VMEM((2, 8, 128), jnp.float32),
            pltpu.VMEM((2, 8, 128), jnp.float32),
            dma((SEQS, 8)),
            dma((SEQS, 8)),
            dma((SEQS, 32)),
            dma((SEQS, 32)),
            dma((32,)),
            dma((32,)),
            dma((2,)),
            dma((2,)),
        ],
        compiler_params=pltpu.CompilerParams(
            collective_id=1, has_side_effects=True, vmem_limit_bytes=32 * 1024 * 1024
        ),
    )(sums, chosen_0, chosen_1)


def body(activations, out_grads, token_mask, row_signs, col_signs, bank, bank_index):
    squared = float(D) * float(D)
    sums = gathered_products(
        activations,
        out_grads,
        row_signs.reshape(1, 256),
        col_signs.reshape(1, FEATS),
        token_mask.reshape(SEQS, 1, TOKENS),
    )
    chosen = [
        lax.dynamic_index_in_dim(bank, bank_index[seq], 0, keepdims=False, allow_negative_indices=False)
        for seq in range(SEQS)
    ]
    prints, totals = mixed_prints(sums, *chosen)
    cross, own, refsq = totals[0:2, 0], totals[2:4, 0], totals[4:6, 0]
    scores = D * (cross / squared) / jnp.sqrt((own / squared + 1e-06) * (refsq / squared + 1e-06))
    return prints, scores


def solution(mesh):
    split = Mesh(mesh.devices.reshape(4, 2, 2, 2, 4), EVERY)
    return jax.shard_map(
        body,
        mesh=split,
        in_specs=(
            P(None, TOK, COL),
            P(None, TOK, COL),
            P(None, TOK),
            P(TOK),
            P(COL),
            P(None, TOK, COL),
            P(),
        ),
        out_specs=(P(None, TOK, COL), P()),
        check_vma=False,
    )
```

```python
import functools
import math

import jax
import jax.numpy as jnp
from jax import lax
from jax.experimental import pallas as pl
from jax.experimental.pallas import tpu as pltpu
from jax.sharding import Mesh
from jax.sharding import PartitionSpec as P

D = 4096
TOK = ("tok_0", "tok_1", "tok_2")
COL = ("col_0", "col_1")
EVERY = ("tok_0", "tok_1", "tok_2", "col_0", "col_1")
MESH = pl.DeviceIdType.MESH

SEQS = 2
TOKENS = 1536
HALF = TOKENS // 2
FEATS = 512
BLOCKS = 4
UNITS = SEQS * BLOCKS * 2

ORDER = (
    ('run', 0, 0, 0),
    ('run', 1, 0, 0),
    ('core', 0, 0, 0),
    ('core', 1, 0, 0),
    ('half', 0, 0, 0),
    ('half', 1, 0, 0),
    ('rpass', 0),
    ('full', 0, 0, 0),
    ('full', 1, 0, 0),
    ('end', 0, 0, 0),
    ('end', 1, 0, 0),
    ('run', 0, 3, 0),
    ('run', 0, 0, 1),
    ('core', 0, 3, 0),
    ('run', 0, 3, 1),
    ('core', 0, 0, 1),
    ('run', 0, 1, 0),
    ('core', 0, 3, 1),
    ('half', 0, 3, 0),
    ('run', 0, 1, 1),
    ('core', 0, 1, 0),
    ('half', 0, 0, 1),
    ('half', 0, 3, 1),
    ('core', 0, 1, 1),
    ('full', 0, 3, 0),
    ('run', 0, 2, 0),
    ('half', 0, 1, 0),
    ('run', 0, 2, 1),
    ('full', 0, 0, 1),
    ('core', 0, 2, 0),
    ('end', 0, 3, 0),
    ('full', 0, 3, 1),
    ('core', 0, 2, 1),
    ('half', 0, 1, 1),
    ('end', 0, 0, 1),
    ('end', 0, 3, 1),
    ('full', 0, 1, 0),
    ('half', 0, 2, 0),
    ('half', 0, 2, 1),
    ('end', 0, 1, 0),
    ('full', 0, 1, 1),
    ('rpass', 1),
    ('run', 1, 0, 1),
    ('full', 0, 2, 0),
    ('end', 0, 1, 1),
    ('full', 0, 2, 1),
    ('core', 1, 0, 1),
    ('end', 0, 2, 0),
    ('end', 0, 2, 1),
    ('half', 1, 0, 1),
    ('full', 1, 0, 1),
    ('run', 1, 3, 0),
    ('run', 1, 3, 1),
    ('core', 1, 3, 0),
    ('run', 1, 1, 0),
    ('core', 1, 3, 1),
    ('run', 1, 1, 1),
    ('core', 1, 1, 0),
    ('half', 1, 3, 0),
    ('end', 1, 0, 1),
    ('mix', 0),
    ('core', 1, 1, 1),
    ('half', 1, 3, 1),
    ('half', 1, 1, 0),
    ('full', 1, 3, 0),
    ('run', 1, 2, 0),
    ('half', 1, 1, 1),
    ('run', 1, 2, 1),
    ('full', 1, 3, 1),
    ('core', 1, 2, 0),
    ('end', 1, 3, 0),
    ('full', 1, 1, 0),
    ('core', 1, 2, 1),
    ('end', 1, 3, 1),
    ('full', 1, 1, 1),
    ('end', 1, 1, 0),
    ('half', 1, 2, 0),
    ('half', 1, 2, 1),
    ('end', 1, 1, 1),
    ('full', 1, 2, 0),
    ('full', 1, 2, 1),
    ('cols', 0),
    ('end', 1, 2, 0),
    ('end', 1, 2, 1),
    ('mix', 1),
    ('land', 0),
    ('cols', 1),
    ('land', 1),
)


def hadamard_rows(first, rows, order):
    down = lax.broadcasted_iota(jnp.int32, (rows, order), 0) + first
    common_bits = jnp.bitwise_and(down, lax.broadcasted_iota(jnp.int32, (rows, order), 1))
    for shift in (8, 4, 2, 1):
        common_bits = jnp.bitwise_xor(common_bits, jnp.right_shift(common_bits, shift))
    return (1 - 2 * jnp.bitwise_and(common_bits, 1)).astype(jnp.float32)


def gather_kernel(
    acts,
    grads,
    row_bits,
    col_bits,
    mask,
    chosen_0,
    chosen_1,
    out,
    totals,
    sums,
    bits,
    walsh,
    tables,
    a_buf,
    m_buf,
    part,
    core_in,
    x_half,
    x_full,
    y_in,
    load_sem,
    a_send,
    a_recv,
    m_send,
    m_recv,
    core_send,
    core_recv,
    xh_send,
    xh_recv,
    xf_send,
    xf_recv,
    y_send,
    y_recv,
    bit_load,
    bit_send,
    bit_recv,
    wide,
    work,
    got,
    ready,
    land,
    mine,
    theirs,
    late,
    col_send,
    col_recv,
    grp_send,
    grp_recv,
    red_send,
    red_recv,
    late_send,
    late_recv,
):
    x = lax.axis_index("tok_0")
    y_lo = lax.axis_index("tok_1")
    core = lax.axis_index("tok_2")
    y_hi = lax.axis_index("col_0")
    z = lax.axis_index("col_1")
    x_next, x_prev, x_far = lax.rem(x + 1, 4), lax.rem(x + 3, 4), lax.rem(x + 2, 4)
    z_ids = ((x, y_lo, core, y_hi, lax.rem(z + 1, 4)), (x, y_lo, core, y_hi, lax.rem(z + 3, 4)))
    x_ids = ((x_next, y_lo, core, y_hi, z), (x_prev, y_lo, core, y_hi, z))
    core_id = (x, y_lo, 1 - core, y_hi, z)
    pair_id = (x, 1 - y_lo, core, y_hi, z)
    far_id = (x, y_lo, core, 1 - y_hi, z)
    last_ids = (far_id, core_id, (x, y_lo, 1 - core, 1 - y_hi, z))
    col_me = y_hi * 4 + z
    grp_me = x * 8 + y_lo * 4 + z

    def col_peer(j):
        there_y = lax.rem(y_hi + lax.div(j, 4), 2)
        there_z = lax.rem(z + j, 4)
        return there_y * 4 + there_z, (x, y_lo, core, there_y, there_z)

    def grp_peer(j):
        there_x = lax.rem(x + lax.div(j, 8), 4)
        there_y = lax.rem(y_lo + lax.div(j, 4), 2)
        there_z = lax.rem(z + j, 4)
        return there_x * 8 + there_y * 4 + there_z, (there_x, there_y, core, y_hi, there_z)

    bit_own = pltpu.make_async_copy(row_bits, bits.at[core, x, y_lo], bit_load)
    m_own = [pltpu.make_async_copy(grads.at[seq], m_buf.at[seq, 0], load_sem.at[seq]) for seq in range(SEQS)]
    a_own = [pltpu.make_async_copy(acts.at[seq], a_buf.at[seq, 0], load_sem.at[2 + seq]) for seq in range(SEQS)]
    for copy in (bit_own, *m_own, *a_own):
        copy.start()

    barrier = pltpu.get_barrier_semaphore()

    @pl.loop(1, 8)
    def _(j):
        pl.semaphore_signal(barrier, inc=1, device_id=col_peer(j)[1], device_id_type=MESH)

    @pl.loop(1, 32)
    def _(j):
        pl.semaphore_signal(barrier, inc=1, device_id=grp_peer(j)[1], device_id_type=MESH)

    for partner in last_ids[1:]:
        pl.semaphore_signal(barrier, inc=1, device_id=partner, device_id_type=MESH)
    pl.semaphore_wait(barrier, 40)

    def rows_of(half):
        return pl.ds(half * HALF, HALF)

    def remote(src, dst, send, recv, device):
        return pltpu.make_async_remote_copy(
            src_ref=src, dst_ref=dst, send_sem=send, recv_sem=recv, device_id=device, device_id_type=MESH
        )

    def ring_copy(seq, way, half, hop):
        slot = (3, 1)[way] if hop == 0 else 2
        index = (seq * 2 + way) * 3 + (2 if hop else half)
        src = acts.at[seq, rows_of(half)] if hop == 0 else a_buf.at[seq, (3, 1)[way], rows_of(half)]
        return remote(src, a_buf.at[seq, slot, rows_of(half)], a_send.at[index], a_recv.at[index], z_ids[way])

    def swap_copy(seq):
        return remote(m_buf.at[seq, 0], m_buf.at[seq, 1], m_send.at[seq], m_recv.at[seq], far_id)

    sent = []

    def start(copy):
        copy.start()
        sent.append(copy)

    def ring_own(seq):
        for step in range(2):
            for way in range(2):
                start(ring_copy(seq, way, (way + step) % 2, 0))

    def ring_pass(seq):
        for way in range(2):
            ring_copy(seq, way, way, 0).wait_recv()
            start(ring_copy(seq, way, way, 1))

    def ring_near(seq, way):
        ring_copy(seq, way, 1 - way, 0).wait_recv()

    def ring_far(seq):
        for way in range(2):
            ring_copy(seq, way, way, 1).wait_recv()

    def bit_copy(index, ref, device):
        return remote(ref, ref, bit_send.at[index], bit_recv.at[index], device)

    def share_bits():
        for way in range(2):
            start(bit_copy(1 + way, bits.at[core, x], x_ids[way]))
        for way in range(2):
            bit_copy(1 + way, bits.at[core, x], x_ids[way]).wait_recv()
        start(bit_copy(3, bits.at[core, x_prev], x_ids[0]))
        bit_copy(3, bits.at[core, x_prev], x_ids[0]).wait_recv()
        start(bit_copy(4, bits.at[core], core_id))

    def sign_tables():
        bit_copy(4, bits.at[core], core_id).wait_recv()

        @pl.loop(0, 8)
        def _(i):
            row = bits[lax.rem(i, 2), 2 * y_hi + lax.div(i, 4), lax.rem(lax.div(i, 2), 2)]
            signs = (2 * row - 1).astype(jnp.float32)
            tables[i] = (walsh[...] * signs).astype(jnp.bfloat16)

    def column_signs(seq):
        signs = (2 * col_bits[...] - 1).astype(jnp.float32).astype(jnp.bfloat16)

        @pl.loop(0, TOKENS // 32)
        def _(i):
            rows = pl.ds(pl.multiple_of(i * 32, 32), 32)
            m_buf[seq, 0, rows] = m_buf[seq, 0, rows] * signs

    core_sign = (1 - 2 * core).astype(jnp.float32)

    def compute(unit, seq, slot, m):
        block = lax.rem(z + slot, 4)
        counted = mask[seq].astype(jnp.float32).astype(jnp.bfloat16)

        @pl.loop(0, 2)
        def _(b):
            columns = pl.ds(pl.multiple_of(b * 256, 256), 256)
            rows_first = a_buf[seq, slot, :, columns].T * counted
            tile = jnp.dot(rows_first, m_buf[seq, m], preferred_element_type=jnp.float32)
            coarse = tile.astype(jnp.bfloat16)
            fine = (tile - coarse.astype(jnp.float32)).astype(jnp.bfloat16)
            table = tables[2 * block + b]
            mixed = jnp.dot(table, coarse, preferred_element_type=jnp.float32)
            mixed += jnp.dot(table, fine, preferred_element_type=jnp.float32)
            part[unit, b] = mixed

        @pl.loop(0, 16)
        def _(i):
            rows = pl.ds(pl.multiple_of(i * 16, 16), 16)
            low = part[unit, 0, rows]
            high = part[unit, 1, rows] * core_sign
            part[unit, 0, rows] = low + high
            part[unit, 1, rows] = low - high

        start(core_copy(unit))

    def core_copy(unit):
        return remote(part.at[unit, 1], core_in.at[unit], core_send.at[unit], core_recv.at[unit], core_id)

    def chunk(unit, x_of):
        return part.at[unit, 0, pl.ds(pl.multiple_of(x_of * 64, 64), 64)]

    def x_half_copy(unit, way):
        rows = pl.ds(pl.multiple_of(x_far * 64 + way * 32, 32), 32)
        index = unit * 2 + way
        return remote(
            part.at[unit, 0, rows], x_half.at[unit, way], xh_send.at[index], xh_recv.at[index], x_ids[way]
        )

    def x_full_copy(unit, way):
        index = unit * 2 + way
        src = chunk(unit, (x_next, x_prev)[way])
        return remote(src, x_full.at[unit, way], xf_send.at[index], xf_recv.at[index], x_ids[way])

    def y_copy(unit):
        rows = pl.ds(pl.multiple_of(x * 64 + (1 - y_lo) * 32, 32), 32)
        return remote(part.at[unit, 0, rows], y_in.at[unit], y_send.at[unit], y_recv.at[unit], pair_id)

    def sum_core(unit):
        core_copy(unit).wait_recv()

        def add(first, rows):
            @pl.loop(0, rows // 8)
            def _(i):
                there = pl.ds(pl.multiple_of(first + i * 8, 8), 8)
                part[unit, 0, there] += core_in[unit, there]

        add(x_far * 64, 64)
        for way in range(2):
            start(x_half_copy(unit, way))
        for other in (x_next, x_prev, x):
            add(other * 64, 64)

    def sum_half(unit):
        for way in range(2):
            x_half_copy(unit, way).wait_recv()
            first = (x_next, x_prev)[way] * 64 + way * 32

            @pl.loop(0, 4)
            def _(i):
                there = pl.ds(pl.multiple_of(first + i * 8, 8), 8)
                part[unit, 0, there] += x_half[unit, way, pl.ds(pl.multiple_of(i * 8, 8), 8)]

            start(x_full_copy(unit, way))

    def sum_full(unit):
        for way in range(2):
            x_full_copy(unit, way).wait_recv()

        @pl.loop(0, 8)
        def _(i):
            there = pl.ds(pl.multiple_of(x * 64 + i * 8, 8), 8)
            here = pl.ds(pl.multiple_of(i * 8, 8), 8)
            part[unit, 0, there] += x_full[unit, 0, here] + x_full[unit, 1, here]

        start(y_copy(unit))

    def finish(unit, seq, slot, m):
        block = lax.rem(z + slot, 4)
        columns = pl.ds(pl.multiple_of(lax.rem(m + y_hi, 2) * FEATS, FEATS), FEATS)
        y_copy(unit).wait_recv()

        @pl.loop(0, 4)
        def _(i):
            here = pl.ds(pl.multiple_of(i * 8, 8), 8)
            there = pl.ds(pl.multiple_of(x * 64 + y_lo * 32 + i * 8, 8), 8)
            sums[seq, block, here, columns] = part[unit, 0, there] + y_in[unit, here]

    def piece(peer):
        return pl.ds(pl.multiple_of(peer * 32, 32), 32)

    def col_copy(seq, j):
        peer, device = col_peer(j)
        return remote(
            work.at[seq, piece(peer)], got.at[seq, col_me], col_send.at[seq, j], col_recv.at[seq, j], device
        )

    def grp_copy(seq, j):
        peer, device = grp_peer(j)
        return remote(
            ready.at[seq, peer], land.at[seq, grp_me], grp_send.at[seq, j], grp_recv.at[seq, j], device
        )

    def red_copy(j):
        return remote(mine, theirs.at[grp_me], red_send.at[j], red_recv.at[j], grp_peer(j)[1])

    last_me = y_hi * 2 + core

    def late_copy(step):
        return remote(
            late.at[4], late.at[last_me], late_send.at[step], late_recv.at[step], last_ids[step]
        )

    def pair(low, high):
        return low + high, low - high

    def four(values):
        a, b = pair(values[0], values[2])
        c, d = pair(values[1], values[3])
        first, second = pair(a, c)
        third, fourth = pair(b, d)
        return first, second, third, fourth

    def mix_local(seq):
        @pl.loop(0, 4)
        def _(q):
            rows = pl.ds(pl.multiple_of(q * 8, 8), 8)
            for half in range(2):
                columns = slice(half * 256, half * 256 + 256)
                upper = slice(512 + half * 256, 768 + half * 256)
                left = four([sums[seq, a, rows, columns] for a in range(4)])
                right = four([sums[seq, a, rows, upper] for a in range(4)])
                for a in range(4):
                    low, high = pair(left[a], right[a])
                    work[seq, pl.ds(pl.multiple_of(q * 32 + a * 8, 8), 8), columns] = low
                    work[seq, pl.ds(pl.multiple_of(128 + q * 32 + a * 8, 8), 8), columns] = high

        values = work[seq]
        coarse = values.astype(jnp.bfloat16)
        fine = (values - coarse.astype(jnp.float32)).astype(jnp.bfloat16)
        mixed = jnp.dot(coarse, wide[...], preferred_element_type=jnp.float32)
        mixed += jnp.dot(fine, wide[...], preferred_element_type=jnp.float32)
        work[seq] = mixed * (1.0 / D)

    def mix_cols(seq):
        @pl.loop(0, 4)
        def _(o):
            for part in range(2):
                columns = slice(part * 256, part * 256 + 256)
                rows = pl.ds(pl.multiple_of(o * 8, 8), 8)
                left = four([got[seq, src, rows, columns] for src in range(4)])
                right = four([got[seq, 4 + src, rows, columns] for src in range(4)])
                for c in range(4):
                    low, high = pair(left[c], right[c])
                    ready[seq, o * 4 + c, :, columns] = low
                    ready[seq, 16 + o * 4 + c, :, columns] = high

    def mix(seq):
        mix_local(seq)

        @pl.loop(1, 8)
        def _(j):
            col_copy(seq, j).start()

        got[seq, col_me] = work[seq, piece(col_me)]

    def trade(seq):
        @pl.loop(1, 8)
        def _(j):
            col_copy(seq, j).wait_recv()

        mix_cols(seq)

        @pl.loop(1, 32)
        def _(j):
            grp_copy(seq, j).start()

        land[seq, grp_me] = ready[seq, grp_me]

    lanes = lax.broadcasted_iota(jnp.int32, (1, 128), 1)

    def score_terms(seq, row):
        @pl.loop(1, 32)
        def _(j):
            grp_copy(seq, j).wait_recv()

        def add(i, carry):
            rows = pl.ds(pl.multiple_of(i * 8, 8), 8)
            value = land[seq, i]
            other = (chosen_0, chosen_1)[seq][rows]
            out[seq, rows] = value
            terms = (value * other, value * value, other * other)
            return tuple(total + term for total, term in zip(carry, terms))

        zero = tuple(jnp.zeros((8, 512), jnp.float32) for _ in range(3))
        for kind, total in enumerate(lax.fori_loop(0, 32, add, zero)):
            total = jnp.sum(jnp.sum(total, axis=1, keepdims=True), axis=0, keepdims=True)
            row = row + jnp.where(lanes == 2 * kind + seq, total, 0.0)
        return row

    ring_own(0)
    walsh[...] = hadamard_rows(0, 256, 256)
    bit_own.wait()
    start(bit_copy(0, bits.at[core, x, y_lo], pair_id))
    m_own[0].wait()
    column_signs(0)
    start(swap_copy(0))
    m_own[1].wait()
    column_signs(1)
    start(swap_copy(1))
    bit_copy(0, bits.at[core, x, y_lo], pair_id).wait_recv()
    share_bits()
    for copy in a_own:
        copy.wait()
    sign_tables()

    @pl.loop(0, 8)
    def _(i):
        rows = pl.ds(pl.multiple_of(i * 64, 64), 64)
        wide[rows] = hadamard_rows(i * 64, 64, 512).astype(jnp.bfloat16)

    row = jnp.zeros((1, 128), jnp.float32)
    here = {("a", 0, 0), ("a", 1, 0), ("m", 0, 0), ("m", 1, 0)}

    def once(key, wait):
        if key not in here:
            here.add(key)
            wait()

    for step, *rest in ORDER:
        if step == "mix":
            mix(rest[0])
            continue
        if step == "cols":
            trade(rest[0])
            continue
        if step == "land":
            row = score_terms(rest[0], row)
            continue
        if step == "rpass":
            ring_pass(rest[0])
            if rest[0] == 0:
                ring_own(1)
            continue
        seq, slot, m = rest
        unit = (seq * BLOCKS + slot) * 2 + m
        if step == "run":
            if slot == 2:
                once(("a", seq, 2), lambda seq=seq: ring_far(seq))
            else:
                once(("a", seq, slot), lambda seq=seq, slot=slot: ring_near(seq, 0 if slot == 3 else 1))
            once(("m", seq, m), lambda seq=seq: swap_copy(seq).wait_recv())
            compute(unit, seq, slot, m)
        elif step == "core":
            sum_core(unit)
        elif step == "half":
            sum_half(unit)
        elif step == "full":
            sum_full(unit)
        else:
            finish(unit, seq, slot, m)
    mine[...] = row

    @pl.loop(1, 32)
    def _(j):
        red_copy(j).start()

    theirs[grp_me] = row

    @pl.loop(1, 32)
    def _(j):
        red_copy(j).wait_recv()

    row = lax.fori_loop(0, 32, lambda i, total: total + theirs[i], jnp.zeros((1, 128), jnp.float32))
    late[4] = row
    for step in range(3):
        late_copy(step).start()
    late[last_me] = row
    for step in range(3):
        late_copy(step).wait_recv()
    totals[...] = (late[0] + late[1]) + (late[2] + late[3])

    for copy in sent:
        copy.wait_send()
    for seq in range(SEQS):

        @pl.loop(1, 8)
        def _(j):
            col_copy(seq, j).wait_send()

        @pl.loop(1, 32)
        def _(j):
            grp_copy(seq, j).wait_send()

    @pl.loop(1, 32)
    def _(j):
        red_copy(j).wait_send()

    for step in range(3):
        late_copy(step).wait_send()


def prints_and_totals(acts, grads, row_bits, col_bits, mask, chosen_0, chosen_1):
    dma = pltpu.SemaphoreType.DMA
    vmem = pl.BlockSpec(memory_space=pltpu.VMEM)
    return pl.pallas_call(
        gather_kernel,
        out_shape=(
            jax.ShapeDtypeStruct((SEQS, 256, FEATS), jnp.float32),
            jax.ShapeDtypeStruct((1, 128), jnp.float32),
        ),
        in_specs=[
            pl.BlockSpec(memory_space=pl.ANY),
            pl.BlockSpec(memory_space=pl.ANY),
            pl.BlockSpec(memory_space=pl.ANY),
            vmem,
            vmem,
            vmem,
            vmem,
        ],
        out_specs=(vmem, vmem),
        scratch_shapes=[
            pltpu.VMEM((SEQS, BLOCKS, 32, 2 * FEATS), jnp.float32),
            pltpu.VMEM((2, 4, 2, 1, 256), jnp.int32),
            pltpu.VMEM((256, 256), jnp.float32),
            pltpu.VMEM((8, 256, 256), jnp.bfloat16),
            pltpu.VMEM((SEQS, BLOCKS, TOKENS, FEATS), jnp.bfloat16),
            pltpu.VMEM((SEQS, 2, TOKENS, FEATS), jnp.bfloat16),
            pltpu.VMEM((UNITS, 2, 256, FEATS), jnp.float32),
            pltpu.VMEM((UNITS, 256, FEATS), jnp.float32),
            pltpu.VMEM((UNITS, 2, 32, FEATS), jnp.float32),
            pltpu.VMEM((UNITS, 2, 64, FEATS), jnp.float32),
            pltpu.VMEM((UNITS, 32, FEATS), jnp.float32),
            dma((4,)),
            dma((12,)),
            dma((12,)),
            dma((2,)),
            dma((2,)),
            dma((UNITS,)),
            dma((UNITS,)),
            dma((2 * UNITS,)),
            dma((2 * UNITS,)),
            dma((2 * UNITS,)),
            dma((2 * UNITS,)),
            dma((UNITS,)),
            dma((UNITS,)),
            dma,
            dma((5,)),
            dma((5,)),
            pltpu.VMEM((512, 512), jnp.bfloat16),
            pltpu.VMEM((SEQS, 256, 512), jnp.float32),
            pltpu.VMEM((SEQS, 8, 32, 512), jnp.float32),
            pltpu.VMEM((SEQS, 32, 8, 512), jnp.float32),
            pltpu.VMEM((SEQS, 32, 8, 512), jnp.float32),
            pltpu.VMEM((1, 128), jnp.float32),
            pltpu.VMEM((32, 1, 128), jnp.float32),
            pltpu.VMEM((5, 1, 128), jnp.float32),
            dma((SEQS, 8)),
            dma((SEQS, 8)),
            dma((SEQS, 32)),
            dma((SEQS, 32)),
            dma((32,)),
            dma((32,)),
            dma((3,)),
            dma((3,)),
        ],
        compiler_params=pltpu.CompilerParams(
            collective_id=0, has_side_effects=True, vmem_limit_bytes=67043328
        ),
    )(acts, grads, row_bits, col_bits, mask, chosen_0, chosen_1)


def body(activations, out_grads, token_mask, row_signs, col_signs, bank, bank_index):
    squared = float(D) * float(D)
    chosen = [
        lax.dynamic_index_in_dim(bank, bank_index[seq], 0, keepdims=False, allow_negative_indices=False)
        for seq in range(SEQS)
    ]
    prints, totals = prints_and_totals(
        activations,
        out_grads,
        row_signs.reshape(1, 256),
        col_signs.reshape(1, FEATS),
        token_mask.reshape(SEQS, 1, TOKENS),
        *chosen,
    )
    cross, own, refsq = totals[0, 0:2], totals[0, 2:4], totals[0, 4:6]
    scores = D * (cross / squared) / jnp.sqrt((own / squared + 1e-06) * (refsq / squared + 1e-06))
    return prints, scores


def solution(mesh):
    split = Mesh(mesh.devices.reshape(4, 2, 2, 2, 4), EVERY)
    return jax.shard_map(
        body,
        mesh=split,
        in_specs=(
            P(None, TOK, COL),
            P(None, TOK, COL),
            P(None, TOK),
            P(TOK),
            P(COL),
            P(None, TOK, COL),
            P(),
        ),
        out_specs=(P(None, TOK, COL), P()),
        check_vma=False,
    )
```

```python
import functools
import math

import jax
import jax.numpy as jnp
from jax import lax
from jax.experimental import pallas as pl
from jax.experimental.pallas import tpu as pltpu
from jax.sharding import Mesh
from jax.sharding import PartitionSpec as P

D = 4096
TOK = ("tok_0", "tok_1", "tok_2")
COL = ("col_0", "col_1")
EVERY = ("tok_0", "tok_1", "tok_2", "col_0", "col_1")
MESH = pl.DeviceIdType.MESH

SEQS = 2
TOKENS = 1536
HALF = TOKENS // 2
FEATS = 512
BLOCKS = 4
UNITS = SEQS * BLOCKS * 2

ORDER = (
    ('run', 0, 0, 0),
    ('run', 1, 0, 0),
    ('core', 0, 0, 0),
    ('core', 1, 0, 0),
    ('half', 0, 0, 0),
    ('half', 1, 0, 0),
    ('spass', 0),
    ('rpass', 0),
    ('full', 0, 0, 0),
    ('full', 1, 0, 0),
    ('run', 0, 3, 0),
    ('run', 0, 0, 1),
    ('core', 0, 3, 0),
    ('run', 0, 3, 1),
    ('core', 0, 0, 1),
    ('run', 0, 1, 0),
    ('half', 0, 3, 0),
    ('core', 0, 3, 1),
    ('run', 0, 1, 1),
    ('half', 0, 0, 1),
    ('core', 0, 1, 0),
    ('core', 0, 1, 1),
    ('full', 0, 3, 0),
    ('half', 0, 3, 1),
    ('run', 0, 2, 0),
    ('spass', 1),
    ('full', 0, 0, 1),
    ('run', 0, 2, 1),
    ('half', 0, 1, 0),
    ('core', 0, 2, 0),
    ('half', 0, 1, 1),
    ('end', 0, 0, 0),
    ('end', 1, 0, 0),
    ('end', 0, 3, 0),
    ('core', 0, 2, 1),
    ('full', 0, 3, 1),
    ('full', 0, 1, 0),
    ('half', 0, 2, 0),
    ('full', 0, 1, 1),
    ('half', 0, 2, 1),
    ('rpass', 1),
    ('full', 0, 2, 0),
    ('full', 0, 2, 1),
    ('run', 1, 0, 1),
    ('end', 0, 0, 1),
    ('end', 0, 3, 1),
    ('core', 1, 0, 1),
    ('end', 0, 1, 0),
    ('end', 0, 1, 1),
    ('end', 0, 2, 0),
    ('half', 1, 0, 1),
    ('end', 0, 2, 1),
    ('run', 1, 3, 0),
    ('full', 1, 0, 1),
    ('run', 1, 3, 1),
    ('core', 1, 3, 0),
    ('run', 1, 1, 0),
    ('core', 1, 3, 1),
    ('run', 1, 1, 1),
    ('half', 1, 3, 0),
    ('core', 1, 1, 0),
    ('end', 1, 0, 1),
    ('half', 1, 3, 1),
    ('core', 1, 1, 1),
    ('full', 1, 3, 0),
    ('half', 1, 1, 0),
    ('run', 1, 2, 0),
    ('run', 1, 2, 1),
    ('full', 1, 3, 1),
    ('half', 1, 1, 1),
    ('core', 1, 2, 0),
    ('end', 1, 3, 0),
    ('core', 1, 2, 1),
    ('full', 1, 1, 0),
    ('end', 1, 3, 1),
    ('full', 1, 1, 1),
    ('end', 1, 1, 0),
    ('half', 1, 2, 0),
    ('half', 1, 2, 1),
    ('end', 1, 1, 1),
    ('full', 1, 2, 0),
    ('full', 1, 2, 1),
    ('end', 1, 2, 0),
    ('end', 1, 2, 1),
)


def hadamard_rows(first, rows, order):
    down = lax.broadcasted_iota(jnp.int32, (rows, order), 0) + first
    common_bits = jnp.bitwise_and(down, lax.broadcasted_iota(jnp.int32, (rows, order), 1))
    for shift in (8, 4, 2, 1):
        common_bits = jnp.bitwise_xor(common_bits, jnp.right_shift(common_bits, shift))
    return (1 - 2 * jnp.bitwise_and(common_bits, 1)).astype(jnp.float32)


def gather_kernel(
    acts,
    grads,
    row_bits,
    col_bits,
    mask,
    out,
    bits,
    walsh,
    tables,
    a_buf,
    m_buf,
    relay,
    part,
    core_in,
    x_half,
    x_full,
    y_in,
    load_sem,
    a_send,
    a_recv,
    m_send,
    m_recv,
    core_send,
    core_recv,
    xh_send,
    xh_recv,
    xf_send,
    xf_recv,
    y_send,
    y_recv,
    bit_load,
    bit_send,
    bit_recv,
):
    x = lax.axis_index("tok_0")
    y_lo = lax.axis_index("tok_1")
    core = lax.axis_index("tok_2")
    y_hi = lax.axis_index("col_0")
    z = lax.axis_index("col_1")
    y = y_hi * 2 + y_lo

    def at_y(value):
        value = lax.rem(value, 4)
        return (x, lax.rem(value, 2), core, lax.div(value, 2), z)

    x_next, x_prev, x_far = lax.rem(x + 1, 4), lax.rem(x + 3, 4), lax.rem(x + 2, 4)
    z_ids = ((x, y_lo, core, y_hi, lax.rem(z + 1, 4)), (x, y_lo, core, y_hi, lax.rem(z + 3, 4)))
    y_ids = (at_y(y + 1), at_y(y + 3))
    x_ids = ((x_next, y_lo, core, y_hi, z), (x_prev, y_lo, core, y_hi, z))
    core_id = (x, y_lo, 1 - core, y_hi, z)
    pair_id = (x, 1 - y_lo, core, y_hi, z)

    bit_own = pltpu.make_async_copy(row_bits, bits.at[core, x, y_lo], bit_load)
    m_own = [pltpu.make_async_copy(grads.at[seq], m_buf.at[seq, 0], load_sem.at[seq]) for seq in range(SEQS)]
    a_own = [pltpu.make_async_copy(acts.at[seq], a_buf.at[seq, 0], load_sem.at[2 + seq]) for seq in range(SEQS)]
    for copy in (bit_own, *m_own, *a_own):
        copy.start()

    barrier = pltpu.get_barrier_semaphore()
    partners = (*z_ids, *y_ids, *x_ids, core_id)
    for partner in partners:
        pl.semaphore_signal(barrier, inc=1, device_id=partner, device_id_type=MESH)
    pl.semaphore_wait(barrier, len(partners))

    def rows_of(half):
        return pl.ds(half * HALF, HALF)

    def remote(src, dst, send, recv, device):
        return pltpu.make_async_remote_copy(
            src_ref=src, dst_ref=dst, send_sem=send, recv_sem=recv, device_id=device, device_id_type=MESH
        )

    def ring_copy(seq, way, half, hop):
        slot = (3, 1)[way] if hop == 0 else 2
        index = (seq * 2 + way) * 3 + (2 if hop else half)
        src = acts.at[seq, rows_of(half)] if hop == 0 else a_buf.at[seq, (3, 1)[way], rows_of(half)]
        return remote(src, a_buf.at[seq, slot, rows_of(half)], a_send.at[index], a_recv.at[index], z_ids[way])

    def swap_copy(seq, way, hop):
        index = (seq * 2 + way) * 2 + hop
        src = relay.at[seq, way] if hop else m_buf.at[seq, 0, rows_of(way)]
        dst = m_buf.at[seq, 1, rows_of(way)] if hop else relay.at[seq, way]
        return remote(src, dst, m_send.at[index], m_recv.at[index], y_ids[way])

    sent = []

    def start(copy):
        copy.start()
        sent.append(copy)

    def ring_own(seq):
        for step in range(2):
            for way in range(2):
                start(ring_copy(seq, way, (way + step) % 2, 0))

    def ring_pass(seq):
        for way in range(2):
            ring_copy(seq, way, way, 0).wait_recv()
            start(ring_copy(seq, way, way, 1))

    def swap_own(seq):
        for way in range(2):
            start(swap_copy(seq, way, 0))

    def swap_pass(seq):
        for way in range(2):
            swap_copy(seq, way, 0).wait_recv()
            start(swap_copy(seq, way, 1))

    def swap_end(seq):
        for way in range(2):
            swap_copy(seq, way, 1).wait_recv()

    def ring_near(seq, way):
        ring_copy(seq, way, 1 - way, 0).wait_recv()

    def ring_far(seq):
        for way in range(2):
            ring_copy(seq, way, way, 1).wait_recv()

    def bit_copy(index, ref, device):
        return remote(ref, ref, bit_send.at[index], bit_recv.at[index], device)

    def share_bits():
        for way in range(2):
            start(bit_copy(1 + way, bits.at[core, x], x_ids[way]))
        for way in range(2):
            bit_copy(1 + way, bits.at[core, x], x_ids[way]).wait_recv()
        start(bit_copy(3, bits.at[core, x_prev], x_ids[0]))
        bit_copy(3, bits.at[core, x_prev], x_ids[0]).wait_recv()
        start(bit_copy(4, bits.at[core], core_id))

    def sign_tables():
        bit_copy(4, bits.at[core], core_id).wait_recv()

        @pl.loop(0, 8)
        def _(i):
            row = bits[lax.rem(i, 2), 2 * y_hi + lax.div(i, 4), lax.rem(lax.div(i, 2), 2)]
            signs = (2 * row - 1).astype(jnp.float32)
            tables[i] = (walsh[...] * signs).astype(jnp.bfloat16)

    def column_signs(seq):
        signs = (2 * col_bits[...] - 1).astype(jnp.float32).astype(jnp.bfloat16)

        @pl.loop(0, TOKENS // 32)
        def _(i):
            rows = pl.ds(pl.multiple_of(i * 32, 32), 32)
            m_buf[seq, 0, rows] = m_buf[seq, 0, rows] * signs

    core_sign = (1 - 2 * core).astype(jnp.float32)

    def compute(unit, seq, slot, m):
        block = lax.rem(z + slot, 4)
        counted = mask[seq : seq + 1, :].astype(jnp.float32).astype(jnp.bfloat16)

        @pl.loop(0, 2)
        def _(b):
            columns = pl.ds(pl.multiple_of(b * 256, 256), 256)
            rows_first = a_buf[seq, slot, :, columns].T * counted
            tile = jnp.dot(rows_first, m_buf[seq, m], preferred_element_type=jnp.float32)
            coarse = tile.astype(jnp.bfloat16)
            fine = (tile - coarse.astype(jnp.float32)).astype(jnp.bfloat16)
            table = tables[2 * block + b]
            mixed = jnp.dot(table, coarse, preferred_element_type=jnp.float32)
            mixed += jnp.dot(table, fine, preferred_element_type=jnp.float32)
            part[unit, b] = mixed

        @pl.loop(0, 16)
        def _(i):
            rows = pl.ds(pl.multiple_of(i * 16, 16), 16)
            low = part[unit, 0, rows]
            high = part[unit, 1, rows] * core_sign
            part[unit, 0, rows] = low + high
            part[unit, 1, rows] = low - high

        start(core_copy(unit))

    def core_copy(unit):
        return remote(part.at[unit, 1], core_in.at[unit], core_send.at[unit], core_recv.at[unit], core_id)

    def chunk(unit, x_of):
        return part.at[unit, 0, pl.ds(pl.multiple_of(x_of * 64, 64), 64)]

    def x_half_copy(unit, way):
        rows = pl.ds(pl.multiple_of(x_far * 64 + way * 32, 32), 32)
        index = unit * 2 + way
        return remote(
            part.at[unit, 0, rows], x_half.at[unit, way], xh_send.at[index], xh_recv.at[index], x_ids[way]
        )

    def x_full_copy(unit, way):
        index = unit * 2 + way
        src = chunk(unit, (x_next, x_prev)[way])
        return remote(src, x_full.at[unit, way], xf_send.at[index], xf_recv.at[index], x_ids[way])

    def y_copy(unit):
        rows = pl.ds(pl.multiple_of(x * 64 + (1 - y_lo) * 32, 32), 32)
        return remote(part.at[unit, 0, rows], y_in.at[unit], y_send.at[unit], y_recv.at[unit], pair_id)

    def sum_core(unit):
        core_copy(unit).wait_recv()

        def add(first, rows):
            @pl.loop(0, rows // 8)
            def _(i):
                there = pl.ds(pl.multiple_of(first + i * 8, 8), 8)
                part[unit, 0, there] += core_in[unit, there]

        add(x_far * 64, 64)
        for way in range(2):
            start(x_half_copy(unit, way))
        for other in (x_next, x_prev, x):
            add(other * 64, 64)

    def sum_half(unit):
        for way in range(2):
            x_half_copy(unit, way).wait_recv()
            first = (x_next, x_prev)[way] * 64 + way * 32

            @pl.loop(0, 4)
            def _(i):
                there = pl.ds(pl.multiple_of(first + i * 8, 8), 8)
                part[unit, 0, there] += x_half[unit, way, pl.ds(pl.multiple_of(i * 8, 8), 8)]

            start(x_full_copy(unit, way))

    def sum_full(unit):
        for way in range(2):
            x_full_copy(unit, way).wait_recv()

        @pl.loop(0, 8)
        def _(i):
            there = pl.ds(pl.multiple_of(x * 64 + i * 8, 8), 8)
            here = pl.ds(pl.multiple_of(i * 8, 8), 8)
            part[unit, 0, there] += x_full[unit, 0, here] + x_full[unit, 1, here]

        start(y_copy(unit))

    def finish(unit, seq, slot, m):
        block = lax.rem(z + slot, 4)
        columns = pl.ds(pl.multiple_of(lax.rem(m + y_hi, 2) * FEATS, FEATS), FEATS)
        y_copy(unit).wait_recv()

        @pl.loop(0, 4)
        def _(i):
            here = pl.ds(pl.multiple_of(i * 8, 8), 8)
            there = pl.ds(pl.multiple_of(x * 64 + y_lo * 32 + i * 8, 8), 8)
            out[seq, block, here, columns] = part[unit, 0, there] + y_in[unit, here]

    ring_own(0)
    walsh[...] = hadamard_rows(0, 256, 256)
    bit_own.wait()
    start(bit_copy(0, bits.at[core, x, y_lo], pair_id))
    m_own[0].wait()
    column_signs(0)
    swap_own(0)
    bit_copy(0, bits.at[core, x, y_lo], pair_id).wait_recv()
    share_bits()
    m_own[1].wait()
    column_signs(1)
    for copy in a_own:
        copy.wait()
    sign_tables()

    here = {("a", 0, 0), ("a", 1, 0), ("m", 0, 0), ("m", 1, 0)}

    def once(key, wait):
        if key not in here:
            here.add(key)
            wait()

    for step, *rest in ORDER:
        if step == "spass":
            swap_pass(rest[0])
            if rest[0] == 0:
                swap_own(1)
            continue
        if step == "rpass":
            ring_pass(rest[0])
            if rest[0] == 0:
                ring_own(1)
            continue
        seq, slot, m = rest
        unit = (seq * BLOCKS + slot) * 2 + m
        if step == "run":
            if slot == 2:
                once(("a", seq, 2), lambda seq=seq: ring_far(seq))
            else:
                once(("a", seq, slot), lambda seq=seq, slot=slot: ring_near(seq, 0 if slot == 3 else 1))
            once(("m", seq, m), lambda seq=seq: swap_end(seq))
            compute(unit, seq, slot, m)
        elif step == "core":
            sum_core(unit)
        elif step == "half":
            sum_half(unit)
        elif step == "full":
            sum_full(unit)
        else:
            finish(unit, seq, slot, m)
    for copy in sent:
        copy.wait_send()


def gathered_products(acts, grads, row_bits, col_bits, mask):
    dma = pltpu.SemaphoreType.DMA
    return pl.pallas_call(
        gather_kernel,
        out_shape=jax.ShapeDtypeStruct((SEQS, BLOCKS, 32, 2 * FEATS), jnp.float32),
        in_specs=[
            pl.BlockSpec(memory_space=pl.ANY),
            pl.BlockSpec(memory_space=pl.ANY),
            pl.BlockSpec(memory_space=pl.ANY),
            pl.BlockSpec(memory_space=pltpu.VMEM),
            pl.BlockSpec(memory_space=pltpu.VMEM),
        ],
        out_specs=pl.BlockSpec(memory_space=pltpu.VMEM),
        scratch_shapes=[
            pltpu.VMEM((2, 4, 2, 1, 256), jnp.int32),
            pltpu.VMEM((256, 256), jnp.float32),
            pltpu.VMEM((8, 256, 256), jnp.bfloat16),
            pltpu.VMEM((SEQS, BLOCKS, TOKENS, FEATS), jnp.bfloat16),
            pltpu.VMEM((SEQS, 2, TOKENS, FEATS), jnp.bfloat16),
            pltpu.VMEM((SEQS, 2, HALF, FEATS), jnp.bfloat16),
            pltpu.VMEM((UNITS, 2, 256, FEATS), jnp.float32),
            pltpu.VMEM((UNITS, 256, FEATS), jnp.float32),
            pltpu.VMEM((UNITS, 2, 32, FEATS), jnp.float32),
            pltpu.VMEM((UNITS, 2, 64, FEATS), jnp.float32),
            pltpu.VMEM((UNITS, 32, FEATS), jnp.float32),
            dma((4,)),
            dma((12,)),
            dma((12,)),
            dma((8,)),
            dma((8,)),
            dma((UNITS,)),
            dma((UNITS,)),
            dma((2 * UNITS,)),
            dma((2 * UNITS,)),
            dma((2 * UNITS,)),
            dma((2 * UNITS,)),
            dma((UNITS,)),
            dma((UNITS,)),
            dma,
            dma((5,)),
            dma((5,)),
        ],
        compiler_params=pltpu.CompilerParams(
            collective_id=0, has_side_effects=True, vmem_limit_bytes=67043328
        ),
    )(acts, grads, row_bits, col_bits, mask)


def mix_kernel(
    sums,
    chosen_0,
    chosen_1,
    out,
    totals,
    walsh,
    work,
    got,
    ready,
    land,
    mine,
    theirs,
    late,
    col_send,
    col_recv,
    grp_send,
    grp_recv,
    red_send,
    red_recv,
    late_send,
    late_recv,
):
    x = lax.axis_index("tok_0")
    y_lo = lax.axis_index("tok_1")
    core = lax.axis_index("tok_2")
    y_hi = lax.axis_index("col_0")
    z = lax.axis_index("col_1")
    col_me = y_hi * 4 + z
    grp_me = x * 8 + y_lo * 4 + z

    def col_peer(j):
        there_y = lax.rem(y_hi + lax.div(j, 4), 2)
        there_z = lax.rem(z + j, 4)
        return there_y * 4 + there_z, (x, y_lo, core, there_y, there_z)

    def grp_peer(j):
        there_x = lax.rem(x + lax.div(j, 8), 4)
        there_y = lax.rem(y_lo + lax.div(j, 4), 2)
        there_z = lax.rem(z + j, 4)
        return there_x * 8 + there_y * 4 + there_z, (there_x, there_y, core, y_hi, there_z)

    core_id = (x, y_lo, 1 - core, y_hi, z)
    far_id = (x, y_lo, core, 1 - y_hi, z)
    last_ids = (far_id, core_id, (x, y_lo, 1 - core, 1 - y_hi, z))
    last_me = y_hi * 2 + core

    barrier = pltpu.get_barrier_semaphore()

    @pl.loop(1, 8)
    def _(j):
        pl.semaphore_signal(barrier, inc=1, device_id=col_peer(j)[1], device_id_type=MESH)

    @pl.loop(1, 32)
    def _(j):
        pl.semaphore_signal(barrier, inc=1, device_id=grp_peer(j)[1], device_id_type=MESH)

    for partner in last_ids[1:]:
        pl.semaphore_signal(barrier, inc=1, device_id=partner, device_id_type=MESH)

    @pl.loop(0, 8)
    def _(i):
        rows = pl.ds(pl.multiple_of(i * 64, 64), 64)
        walsh[rows] = hadamard_rows(i * 64, 64, 512).astype(jnp.bfloat16)

    def remote(src, dst, send, recv, device):
        return pltpu.make_async_remote_copy(
            src_ref=src, dst_ref=dst, send_sem=send, recv_sem=recv, device_id=device, device_id_type=MESH
        )

    def piece(peer):
        return pl.ds(pl.multiple_of(peer * 32, 32), 32)

    def col_copy(seq, j):
        peer, device = col_peer(j)
        return remote(
            work.at[seq, piece(peer)], got.at[seq, col_me], col_send.at[seq, j], col_recv.at[seq, j], device
        )

    def grp_copy(seq, j):
        peer, device = grp_peer(j)
        return remote(
            ready.at[seq, peer], land.at[seq, grp_me], grp_send.at[seq, j], grp_recv.at[seq, j], device
        )

    def red_copy(j):
        return remote(mine, theirs.at[grp_me], red_send.at[j], red_recv.at[j], grp_peer(j)[1])

    def late_copy(step):
        return remote(late.at[4], late.at[last_me], late_send.at[step], late_recv.at[step], last_ids[step])

    def pair(low, high):
        return low + high, low - high

    def four(values):
        a, b = pair(values[0], values[2])
        c, d = pair(values[1], values[3])
        first, second = pair(a, c)
        third, fourth = pair(b, d)
        return first, second, third, fourth

    def mix_local(seq):
        @pl.loop(0, 4)
        def _(q):
            rows = pl.ds(pl.multiple_of(q * 8, 8), 8)
            for half in range(2):
                columns = slice(half * 256, half * 256 + 256)
                upper = slice(512 + half * 256, 768 + half * 256)
                left = four([sums[seq, a, rows, columns] for a in range(4)])
                right = four([sums[seq, a, rows, upper] for a in range(4)])
                for a in range(4):
                    low, high = pair(left[a], right[a])
                    work[seq, pl.ds(pl.multiple_of(q * 32 + a * 8, 8), 8), columns] = low
                    work[seq, pl.ds(pl.multiple_of(128 + q * 32 + a * 8, 8), 8), columns] = high

        values = work[seq]
        coarse = values.astype(jnp.bfloat16)
        fine = (values - coarse.astype(jnp.float32)).astype(jnp.bfloat16)
        mixed = jnp.dot(coarse, walsh[...], preferred_element_type=jnp.float32)
        mixed += jnp.dot(fine, walsh[...], preferred_element_type=jnp.float32)
        work[seq] = mixed * (1.0 / D)

    def mix_cols(seq):
        @pl.loop(0, 4)
        def _(o):
            for part in range(2):
                columns = slice(part * 256, part * 256 + 256)
                rows = pl.ds(pl.multiple_of(o * 8, 8), 8)
                left = four([got[seq, src, rows, columns] for src in range(4)])
                right = four([got[seq, 4 + src, rows, columns] for src in range(4)])
                for c in range(4):
                    low, high = pair(left[c], right[c])
                    ready[seq, o * 4 + c, :, columns] = low
                    ready[seq, 16 + o * 4 + c, :, columns] = high

    for seq in range(SEQS):
        mix_local(seq)
        if seq == 0:
            pl.semaphore_wait(barrier, 40)

        @pl.loop(1, 8)
        def _(j):
            col_copy(seq, j).start()

        got[seq, col_me] = work[seq, piece(col_me)]

    for seq in range(SEQS):

        @pl.loop(1, 8)
        def _(j):
            col_copy(seq, j).wait_recv()

        mix_cols(seq)

        @pl.loop(1, 32)
        def _(j):
            grp_copy(seq, j).start()

        land[seq, grp_me] = ready[seq, grp_me]

    lanes = lax.broadcasted_iota(jnp.int32, (1, 128), 1)
    row = jnp.zeros((1, 128), jnp.float32)
    for seq in range(SEQS):

        @pl.loop(1, 32)
        def _(j):
            grp_copy(seq, j).wait_recv()

        def add(i, carry):
            rows = pl.ds(pl.multiple_of(i * 8, 8), 8)
            value = land[seq, i]
            other = (chosen_0, chosen_1)[seq][rows]
            out[seq, rows] = value
            terms = (value * other, value * value, other * other)
            return tuple(total + term for total, term in zip(carry, terms))

        start = tuple(jnp.zeros((8, 512), jnp.float32) for _ in range(3))
        for kind, total in enumerate(lax.fori_loop(0, 32, add, start)):
            total = jnp.sum(jnp.sum(total, axis=1, keepdims=True), axis=0, keepdims=True)
            row = row + jnp.where(lanes == 2 * kind + seq, total, 0.0)

    mine[...] = row

    @pl.loop(1, 32)
    def _(j):
        red_copy(j).start()

    theirs[grp_me] = row

    @pl.loop(1, 32)
    def _(j):
        red_copy(j).wait_recv()

    row = lax.fori_loop(0, 32, lambda i, total: total + theirs[i], jnp.zeros((1, 128), jnp.float32))
    late[4] = row
    for step in range(3):
        late_copy(step).start()
    late[last_me] = row
    for step in range(3):
        late_copy(step).wait_recv()
    totals[...] = (late[0] + late[1]) + (late[2] + late[3])

    for seq in range(SEQS):

        @pl.loop(1, 8)
        def _(j):
            col_copy(seq, j).wait_send()

        @pl.loop(1, 32)
        def _(j):
            grp_copy(seq, j).wait_send()

    @pl.loop(1, 32)
    def _(j):
        red_copy(j).wait_send()

    for step in range(3):
        late_copy(step).wait_send()


def mixed_prints(sums, chosen_0, chosen_1):
    dma = pltpu.SemaphoreType.DMA
    vmem = pl.BlockSpec(memory_space=pltpu.VMEM)
    return pl.pallas_call(
        mix_kernel,
        out_shape=(
            jax.ShapeDtypeStruct((SEQS, 256, 512), jnp.float32),
            jax.ShapeDtypeStruct((1, 128), jnp.float32),
        ),
        in_specs=[vmem, vmem, vmem],
        out_specs=(vmem, vmem),
        scratch_shapes=[
            pltpu.VMEM((512, 512), jnp.bfloat16),
            pltpu.VMEM((SEQS, 256, 512), jnp.float32),
            pltpu.VMEM((SEQS, 8, 32, 512), jnp.float32),
            pltpu.VMEM((SEQS, 32, 8, 512), jnp.float32),
            pltpu.VMEM((SEQS, 32, 8, 512), jnp.float32),
            pltpu.VMEM((1, 128), jnp.float32),
            pltpu.VMEM((32, 1, 128), jnp.float32),
            pltpu.VMEM((5, 1, 128), jnp.float32),
            dma((SEQS, 8)),
            dma((SEQS, 8)),
            dma((SEQS, 32)),
            dma((SEQS, 32)),
            dma((32,)),
            dma((32,)),
            dma((3,)),
            dma((3,)),
        ],
        compiler_params=pltpu.CompilerParams(
            collective_id=1, has_side_effects=True, vmem_limit_bytes=32 * 1024 * 1024
        ),
    )(sums, chosen_0, chosen_1)


def body(activations, out_grads, token_mask, row_signs, col_signs, bank, bank_index):
    squared = float(D) * float(D)
    sums = gathered_products(
        activations,
        out_grads,
        row_signs.reshape(1, 256),
        col_signs.reshape(1, FEATS),
        token_mask,
    )
    chosen = [
        lax.dynamic_index_in_dim(bank, bank_index[seq], 0, keepdims=False, allow_negative_indices=False)
        for seq in range(SEQS)
    ]
    prints, totals = mixed_prints(sums, *chosen)
    cross, own, refsq = totals[0, 0:2], totals[0, 2:4], totals[0, 4:6]
    scores = D * (cross / squared) / jnp.sqrt((own / squared + 1e-06) * (refsq / squared + 1e-06))
    return prints, scores


def solution(mesh):
    split = Mesh(mesh.devices.reshape(4, 2, 2, 2, 4), EVERY)
    return jax.shard_map(
        body,
        mesh=split,
        in_specs=(
            P(None, TOK, COL),
            P(None, TOK, COL),
            P(None, TOK),
            P(TOK),
            P(COL),
            P(None, TOK, COL),
            P(),
        ),
        out_specs=(P(None, TOK, COL), P()),
        check_vma=False,
    )
```

```python
import functools
import math

import jax
import jax.numpy as jnp
from jax import lax
from jax.experimental import pallas as pl
from jax.experimental.pallas import tpu as pltpu
from jax.sharding import Mesh
from jax.sharding import PartitionSpec as P

D = 4096
TOK = ("tok_0", "tok_1", "tok_2")
COL = ("col_0", "col_1")
EVERY = ("tok_0", "tok_1", "tok_2", "col_0", "col_1")
MESH = pl.DeviceIdType.MESH

SEQS = 2
TOKENS = 1536
HALF = TOKENS // 2
FEATS = 512
BLOCKS = 4
UNITS = SEQS * BLOCKS * 2

ORDER = (
    ('run', 0, 0, 0),
    ('run', 1, 0, 0),
    ('core', 0, 0, 0),
    ('core', 1, 0, 0),
    ('half', 0, 0, 0),
    ('half', 1, 0, 0),
    ('spass', 0),
    ('rpass', 0),
    ('full', 0, 0, 0),
    ('full', 1, 0, 0),
    ('run', 0, 3, 0),
    ('run', 0, 0, 1),
    ('core', 0, 3, 0),
    ('run', 0, 3, 1),
    ('core', 0, 0, 1),
    ('run', 0, 1, 0),
    ('half', 0, 3, 0),
    ('core', 0, 3, 1),
    ('run', 0, 1, 1),
    ('half', 0, 0, 1),
    ('core', 0, 1, 0),
    ('core', 0, 1, 1),
    ('full', 0, 3, 0),
    ('half', 0, 3, 1),
    ('run', 0, 2, 0),
    ('spass', 1),
    ('full', 0, 0, 1),
    ('run', 0, 2, 1),
    ('half', 0, 1, 0),
    ('core', 0, 2, 0),
    ('half', 0, 1, 1),
    ('end', 0, 0, 0),
    ('end', 1, 0, 0),
    ('end', 0, 3, 0),
    ('core', 0, 2, 1),
    ('full', 0, 3, 1),
    ('full', 0, 1, 0),
    ('half', 0, 2, 0),
    ('full', 0, 1, 1),
    ('half', 0, 2, 1),
    ('rpass', 1),
    ('full', 0, 2, 0),
    ('full', 0, 2, 1),
    ('run', 1, 0, 1),
    ('end', 0, 0, 1),
    ('end', 0, 3, 1),
    ('core', 1, 0, 1),
    ('end', 0, 1, 0),
    ('end', 0, 1, 1),
    ('end', 0, 2, 0),
    ('half', 1, 0, 1),
    ('end', 0, 2, 1),
    ('run', 1, 3, 0),
    ('full', 1, 0, 1),
    ('run', 1, 3, 1),
    ('core', 1, 3, 0),
    ('run', 1, 1, 0),
    ('core', 1, 3, 1),
    ('run', 1, 1, 1),
    ('half', 1, 3, 0),
    ('core', 1, 1, 0),
    ('end', 1, 0, 1),
    ('half', 1, 3, 1),
    ('core', 1, 1, 1),
    ('full', 1, 3, 0),
    ('half', 1, 1, 0),
    ('run', 1, 2, 0),
    ('run', 1, 2, 1),
    ('full', 1, 3, 1),
    ('half', 1, 1, 1),
    ('core', 1, 2, 0),
    ('end', 1, 3, 0),
    ('core', 1, 2, 1),
    ('full', 1, 1, 0),
    ('end', 1, 3, 1),
    ('full', 1, 1, 1),
    ('end', 1, 1, 0),
    ('half', 1, 2, 0),
    ('half', 1, 2, 1),
    ('end', 1, 1, 1),
    ('full', 1, 2, 0),
    ('full', 1, 2, 1),
    ('end', 1, 2, 0),
    ('end', 1, 2, 1),
)


def hadamard_rows(first, rows, order):
    down = lax.broadcasted_iota(jnp.int32, (rows, order), 0) + first
    common_bits = jnp.bitwise_and(down, lax.broadcasted_iota(jnp.int32, (rows, order), 1))
    for shift in (8, 4, 2, 1):
        common_bits = jnp.bitwise_xor(common_bits, jnp.right_shift(common_bits, shift))
    return (1 - 2 * jnp.bitwise_and(common_bits, 1)).astype(jnp.float32)


def gather_kernel(
    acts,
    grads,
    row_bits,
    col_bits,
    mask,
    out,
    bits,
    walsh,
    tables,
    a_buf,
    m_buf,
    relay,
    part,
    core_in,
    x_half,
    x_full,
    y_in,
    load_sem,
    a_send,
    a_recv,
    m_send,
    m_recv,
    core_send,
    core_recv,
    xh_send,
    xh_recv,
    xf_send,
    xf_recv,
    y_send,
    y_recv,
    bit_load,
    bit_send,
    bit_recv,
):
    x = lax.axis_index("tok_0")
    y_lo = lax.axis_index("tok_1")
    core = lax.axis_index("tok_2")
    y_hi = lax.axis_index("col_0")
    z = lax.axis_index("col_1")
    y = y_hi * 2 + y_lo

    def at_y(value):
        value = lax.rem(value, 4)
        return (x, lax.rem(value, 2), core, lax.div(value, 2), z)

    x_next, x_prev, x_far = lax.rem(x + 1, 4), lax.rem(x + 3, 4), lax.rem(x + 2, 4)
    z_ids = ((x, y_lo, core, y_hi, lax.rem(z + 1, 4)), (x, y_lo, core, y_hi, lax.rem(z + 3, 4)))
    y_ids = (at_y(y + 1), at_y(y + 3))
    x_ids = ((x_next, y_lo, core, y_hi, z), (x_prev, y_lo, core, y_hi, z))
    core_id = (x, y_lo, 1 - core, y_hi, z)
    pair_id = (x, 1 - y_lo, core, y_hi, z)

    bit_own = pltpu.make_async_copy(row_bits, bits.at[core, x, y_lo], bit_load)
    m_own = [pltpu.make_async_copy(grads.at[seq], m_buf.at[seq, 0], load_sem.at[seq]) for seq in range(SEQS)]
    a_own = [pltpu.make_async_copy(acts.at[seq], a_buf.at[seq, 0], load_sem.at[2 + seq]) for seq in range(SEQS)]
    for copy in (bit_own, *m_own, *a_own):
        copy.start()

    barrier = pltpu.get_barrier_semaphore()
    partners = (*z_ids, *y_ids, *x_ids, core_id)
    for partner in partners:
        pl.semaphore_signal(barrier, inc=1, device_id=partner, device_id_type=MESH)
    pl.semaphore_wait(barrier, len(partners))

    def rows_of(half):
        return pl.ds(half * HALF, HALF)

    def remote(src, dst, send, recv, device):
        return pltpu.make_async_remote_copy(
            src_ref=src, dst_ref=dst, send_sem=send, recv_sem=recv, device_id=device, device_id_type=MESH
        )

    def ring_copy(seq, way, half, hop):
        slot = (3, 1)[way] if hop == 0 else 2
        index = (seq * 2 + way) * 3 + (2 if hop else half)
        src = acts.at[seq, rows_of(half)] if hop == 0 else a_buf.at[seq, (3, 1)[way], rows_of(half)]
        return remote(src, a_buf.at[seq, slot, rows_of(half)], a_send.at[index], a_recv.at[index], z_ids[way])

    def swap_copy(seq, way, hop):
        index = (seq * 2 + way) * 2 + hop
        src = relay.at[seq, way] if hop else m_buf.at[seq, 0, rows_of(way)]
        dst = m_buf.at[seq, 1, rows_of(way)] if hop else relay.at[seq, way]
        return remote(src, dst, m_send.at[index], m_recv.at[index], y_ids[way])

    sent = []

    def start(copy):
        copy.start()
        sent.append(copy)

    def ring_own(seq):
        for step in range(2):
            for way in range(2):
                start(ring_copy(seq, way, (way + step) % 2, 0))

    def ring_pass(seq):
        for way in range(2):
            ring_copy(seq, way, way, 0).wait_recv()
            start(ring_copy(seq, way, way, 1))

    def swap_own(seq):
        for way in range(2):
            start(swap_copy(seq, way, 0))

    def swap_pass(seq):
        for way in range(2):
            swap_copy(seq, way, 0).wait_recv()
            start(swap_copy(seq, way, 1))

    def swap_end(seq):
        for way in range(2):
            swap_copy(seq, way, 1).wait_recv()

    def ring_near(seq, way):
        ring_copy(seq, way, 1 - way, 0).wait_recv()

    def ring_far(seq):
        for way in range(2):
            ring_copy(seq, way, way, 1).wait_recv()

    def bit_copy(index, ref, device):
        return remote(ref, ref, bit_send.at[index], bit_recv.at[index], device)

    def share_bits():
        for way in range(2):
            start(bit_copy(1 + way, bits.at[core, x], x_ids[way]))
        for way in range(2):
            bit_copy(1 + way, bits.at[core, x], x_ids[way]).wait_recv()
        start(bit_copy(3, bits.at[core, x_prev], x_ids[0]))
        bit_copy(3, bits.at[core, x_prev], x_ids[0]).wait_recv()
        start(bit_copy(4, bits.at[core], core_id))

    def sign_tables():
        bit_copy(4, bits.at[core], core_id).wait_recv()

        @pl.loop(0, 8)
        def _(i):
            row = bits[lax.rem(i, 2), 2 * y_hi + lax.div(i, 4), lax.rem(lax.div(i, 2), 2)]
            signs = (2 * row - 1).astype(jnp.float32)
            tables[i] = (walsh[...] * signs).astype(jnp.bfloat16)

    def column_signs(seq):
        signs = (2 * col_bits[...] - 1).astype(jnp.float32).astype(jnp.bfloat16)

        @pl.loop(0, TOKENS // 32)
        def _(i):
            rows = pl.ds(pl.multiple_of(i * 32, 32), 32)
            m_buf[seq, 0, rows] = m_buf[seq, 0, rows] * signs

    core_sign = (1 - 2 * core).astype(jnp.float32)

    def compute(unit, seq, slot, m):
        block = lax.rem(z + slot, 4)
        counted = mask[seq : seq + 1, :].astype(jnp.float32).astype(jnp.bfloat16)

        @pl.loop(0, 2)
        def _(b):
            columns = pl.ds(pl.multiple_of(b * 256, 256), 256)
            rows_first = a_buf[seq, slot, :, columns].T * counted
            tile = jnp.dot(rows_first, m_buf[seq, m], preferred_element_type=jnp.float32)
            coarse = tile.astype(jnp.bfloat16)
            fine = (tile - coarse.astype(jnp.float32)).astype(jnp.bfloat16)
            table = tables[2 * block + b]
            mixed = jnp.dot(table, coarse, preferred_element_type=jnp.float32)
            mixed += jnp.dot(table, fine, preferred_element_type=jnp.float32)
            part[unit, b] = mixed

        @pl.loop(0, 16)
        def _(i):
            rows = pl.ds(pl.multiple_of(i * 16, 16), 16)
            low = part[unit, 0, rows]
            high = part[unit, 1, rows] * core_sign
            part[unit, 0, rows] = low + high
            part[unit, 1, rows] = low - high

        start(core_copy(unit))

    def core_copy(unit):
        return remote(part.at[unit, 1], core_in.at[unit], core_send.at[unit], core_recv.at[unit], core_id)

    def chunk(unit, x_of):
        return part.at[unit, 0, pl.ds(pl.multiple_of(x_of * 64, 64), 64)]

    def x_half_copy(unit, way):
        rows = pl.ds(pl.multiple_of(x_far * 64 + way * 32, 32), 32)
        index = unit * 2 + way
        return remote(
            part.at[unit, 0, rows], x_half.at[unit, way], xh_send.at[index], xh_recv.at[index], x_ids[way]
        )

    def x_full_copy(unit, way):
        index = unit * 2 + way
        src = chunk(unit, (x_next, x_prev)[way])
        return remote(src, x_full.at[unit, way], xf_send.at[index], xf_recv.at[index], x_ids[way])

    def y_copy(unit):
        rows = pl.ds(pl.multiple_of(x * 64 + (1 - y_lo) * 32, 32), 32)
        return remote(part.at[unit, 0, rows], y_in.at[unit], y_send.at[unit], y_recv.at[unit], pair_id)

    def sum_core(unit):
        core_copy(unit).wait_recv()

        def add(first, rows):
            @pl.loop(0, rows // 8)
            def _(i):
                there = pl.ds(pl.multiple_of(first + i * 8, 8), 8)
                part[unit, 0, there] += core_in[unit, there]

        add(x_far * 64, 64)
        for way in range(2):
            start(x_half_copy(unit, way))
        for other in (x_next, x_prev, x):
            add(other * 64, 64)

    def sum_half(unit):
        for way in range(2):
            x_half_copy(unit, way).wait_recv()
            first = (x_next, x_prev)[way] * 64 + way * 32

            @pl.loop(0, 4)
            def _(i):
                there = pl.ds(pl.multiple_of(first + i * 8, 8), 8)
                part[unit, 0, there] += x_half[unit, way, pl.ds(pl.multiple_of(i * 8, 8), 8)]

            start(x_full_copy(unit, way))

    def sum_full(unit):
        for way in range(2):
            x_full_copy(unit, way).wait_recv()

        @pl.loop(0, 8)
        def _(i):
            there = pl.ds(pl.multiple_of(x * 64 + i * 8, 8), 8)
            here = pl.ds(pl.multiple_of(i * 8, 8), 8)
            part[unit, 0, there] += x_full[unit, 0, here] + x_full[unit, 1, here]

        start(y_copy(unit))

    def finish(unit, seq, slot, m):
        block = lax.rem(z + slot, 4)
        columns = pl.ds(pl.multiple_of(lax.rem(m + y_hi, 2) * FEATS, FEATS), FEATS)
        y_copy(unit).wait_recv()

        @pl.loop(0, 4)
        def _(i):
            here = pl.ds(pl.multiple_of(i * 8, 8), 8)
            there = pl.ds(pl.multiple_of(x * 64 + y_lo * 32 + i * 8, 8), 8)
            out[seq, block, here, columns] = part[unit, 0, there] + y_in[unit, here]

    ring_own(0)
    walsh[...] = hadamard_rows(0, 256, 256)
    bit_own.wait()
    start(bit_copy(0, bits.at[core, x, y_lo], pair_id))
    m_own[0].wait()
    column_signs(0)
    swap_own(0)
    bit_copy(0, bits.at[core, x, y_lo], pair_id).wait_recv()
    share_bits()
    m_own[1].wait()
    column_signs(1)
    for copy in a_own:
        copy.wait()
    sign_tables()

    here = {("a", 0, 0), ("a", 1, 0), ("m", 0, 0), ("m", 1, 0)}

    def once(key, wait):
        if key not in here:
            here.add(key)
            wait()

    for step, *rest in ORDER:
        if step == "spass":
            swap_pass(rest[0])
            if rest[0] == 0:
                swap_own(1)
            continue
        if step == "rpass":
            ring_pass(rest[0])
            if rest[0] == 0:
                ring_own(1)
            continue
        seq, slot, m = rest
        unit = (seq * BLOCKS + slot) * 2 + m
        if step == "run":
            if slot == 2:
                once(("a", seq, 2), lambda seq=seq: ring_far(seq))
            else:
                once(("a", seq, slot), lambda seq=seq, slot=slot: ring_near(seq, 0 if slot == 3 else 1))
            once(("m", seq, m), lambda seq=seq: swap_end(seq))
            compute(unit, seq, slot, m)
        elif step == "core":
            sum_core(unit)
        elif step == "half":
            sum_half(unit)
        elif step == "full":
            sum_full(unit)
        else:
            finish(unit, seq, slot, m)
    for copy in sent:
        copy.wait_send()


def gathered_products(acts, grads, row_bits, col_bits, mask):
    dma = pltpu.SemaphoreType.DMA
    return pl.pallas_call(
        gather_kernel,
        out_shape=jax.ShapeDtypeStruct((SEQS, BLOCKS, 32, 2 * FEATS), jnp.float32),
        in_specs=[
            pl.BlockSpec(memory_space=pl.ANY),
            pl.BlockSpec(memory_space=pl.ANY),
            pl.BlockSpec(memory_space=pl.ANY),
            pl.BlockSpec(memory_space=pltpu.VMEM),
            pl.BlockSpec(memory_space=pltpu.VMEM),
        ],
        out_specs=pl.BlockSpec(memory_space=pltpu.VMEM),
        scratch_shapes=[
            pltpu.VMEM((2, 4, 2, 1, 256), jnp.int32),
            pltpu.VMEM((256, 256), jnp.float32),
            pltpu.VMEM((8, 256, 256), jnp.bfloat16),
            pltpu.VMEM((SEQS, BLOCKS, TOKENS, FEATS), jnp.bfloat16),
            pltpu.VMEM((SEQS, 2, TOKENS, FEATS), jnp.bfloat16),
            pltpu.VMEM((SEQS, 2, HALF, FEATS), jnp.bfloat16),
            pltpu.VMEM((UNITS, 2, 256, FEATS), jnp.float32),
            pltpu.VMEM((UNITS, 256, FEATS), jnp.float32),
            pltpu.VMEM((UNITS, 2, 32, FEATS), jnp.float32),
            pltpu.VMEM((UNITS, 2, 64, FEATS), jnp.float32),
            pltpu.VMEM((UNITS, 32, FEATS), jnp.float32),
            dma((4,)),
            dma((12,)),
            dma((12,)),
            dma((8,)),
            dma((8,)),
            dma((UNITS,)),
            dma((UNITS,)),
            dma((2 * UNITS,)),
            dma((2 * UNITS,)),
            dma((2 * UNITS,)),
            dma((2 * UNITS,)),
            dma((UNITS,)),
            dma((UNITS,)),
            dma,
            dma((5,)),
            dma((5,)),
        ],
        compiler_params=pltpu.CompilerParams(
            collective_id=0, has_side_effects=True, vmem_limit_bytes=67043328
        ),
    )(acts, grads, row_bits, col_bits, mask)


def mix_kernel(
    sums_there,
    bank_there,
    index,
    out,
    totals,
    sums,
    bank,
    walsh,
    work,
    got,
    ready,
    land,
    mine,
    theirs,
    late,
    col_send,
    col_recv,
    grp_send,
    grp_recv,
    red_send,
    red_recv,
    late_send,
    late_recv,
    load_sem,
):
    x = lax.axis_index("tok_0")
    y_lo = lax.axis_index("tok_1")
    core = lax.axis_index("tok_2")
    y_hi = lax.axis_index("col_0")
    z = lax.axis_index("col_1")
    col_me = y_hi * 4 + z
    grp_me = x * 8 + y_lo * 4 + z

    def col_peer(j):
        there_y = lax.rem(y_hi + lax.div(j, 4), 2)
        there_z = lax.rem(z + j, 4)
        return there_y * 4 + there_z, (x, y_lo, core, there_y, there_z)

    def grp_peer(j):
        there_x = lax.rem(x + lax.div(j, 8), 4)
        there_y = lax.rem(y_lo + lax.div(j, 4), 2)
        there_z = lax.rem(z + j, 4)
        return there_x * 8 + there_y * 4 + there_z, (there_x, there_y, core, y_hi, there_z)

    core_id = (x, y_lo, 1 - core, y_hi, z)
    far_id = (x, y_lo, core, 1 - y_hi, z)
    last_ids = (far_id, core_id, (x, y_lo, 1 - core, 1 - y_hi, z))
    last_me = y_hi * 2 + core

    sums_load = pltpu.make_async_copy(sums_there, sums, load_sem.at[0])
    bank_load = pltpu.make_async_copy(bank_there, bank, load_sem.at[1])
    sums_load.start()
    bank_load.start()
    barrier = pltpu.get_barrier_semaphore()

    @pl.loop(1, 8)
    def _(j):
        pl.semaphore_signal(barrier, inc=1, device_id=col_peer(j)[1], device_id_type=MESH)

    @pl.loop(1, 32)
    def _(j):
        pl.semaphore_signal(barrier, inc=1, device_id=grp_peer(j)[1], device_id_type=MESH)

    for partner in last_ids[1:]:
        pl.semaphore_signal(barrier, inc=1, device_id=partner, device_id_type=MESH)

    @pl.loop(0, 8)
    def _(i):
        rows = pl.ds(pl.multiple_of(i * 64, 64), 64)
        walsh[rows] = hadamard_rows(i * 64, 64, 512).astype(jnp.bfloat16)

    def remote(src, dst, send, recv, device):
        return pltpu.make_async_remote_copy(
            src_ref=src, dst_ref=dst, send_sem=send, recv_sem=recv, device_id=device, device_id_type=MESH
        )

    def piece(peer):
        return pl.ds(pl.multiple_of(peer * 32, 32), 32)

    def col_copy(seq, j):
        peer, device = col_peer(j)
        return remote(
            work.at[seq, piece(peer)], got.at[seq, col_me], col_send.at[seq, j], col_recv.at[seq, j], device
        )

    def grp_copy(seq, j):
        peer, device = grp_peer(j)
        return remote(
            ready.at[seq, peer], land.at[seq, grp_me], grp_send.at[seq, j], grp_recv.at[seq, j], device
        )

    def red_copy(j):
        return remote(mine, theirs.at[grp_me], red_send.at[j], red_recv.at[j], grp_peer(j)[1])

    def late_copy(step):
        return remote(late.at[4], late.at[last_me], late_send.at[step], late_recv.at[step], last_ids[step])

    def pair(low, high):
        return low + high, low - high

    def four(values):
        a, b = pair(values[0], values[2])
        c, d = pair(values[1], values[3])
        first, second = pair(a, c)
        third, fourth = pair(b, d)
        return first, second, third, fourth

    def mix_local(seq):
        @pl.loop(0, 4)
        def _(q):
            rows = pl.ds(pl.multiple_of(q * 8, 8), 8)
            for half in range(2):
                columns = slice(half * 256, half * 256 + 256)
                upper = slice(512 + half * 256, 768 + half * 256)
                left = four([sums[seq, a, rows, columns] for a in range(4)])
                right = four([sums[seq, a, rows, upper] for a in range(4)])
                for a in range(4):
                    low, high = pair(left[a], right[a])
                    work[seq, pl.ds(pl.multiple_of(q * 32 + a * 8, 8), 8), columns] = low
                    work[seq, pl.ds(pl.multiple_of(128 + q * 32 + a * 8, 8), 8), columns] = high

        values = work[seq]
        coarse = values.astype(jnp.bfloat16)
        fine = (values - coarse.astype(jnp.float32)).astype(jnp.bfloat16)
        mixed = jnp.dot(coarse, walsh[...], preferred_element_type=jnp.float32)
        mixed += jnp.dot(fine, walsh[...], preferred_element_type=jnp.float32)
        work[seq] = mixed * (1.0 / D)

    def mix_cols(seq):
        @pl.loop(0, 4)
        def _(o):
            for part in range(2):
                columns = slice(part * 256, part * 256 + 256)
                rows = pl.ds(pl.multiple_of(o * 8, 8), 8)
                left = four([got[seq, src, rows, columns] for src in range(4)])
                right = four([got[seq, 4 + src, rows, columns] for src in range(4)])
                for c in range(4):
                    low, high = pair(left[c], right[c])
                    ready[seq, o * 4 + c, :, columns] = low
                    ready[seq, 16 + o * 4 + c, :, columns] = high

    sums_load.wait()
    for seq in range(SEQS):
        mix_local(seq)
        if seq == 0:
            pl.semaphore_wait(barrier, 40)

        @pl.loop(1, 8)
        def _(j):
            col_copy(seq, j).start()

        got[seq, col_me] = work[seq, piece(col_me)]

    for seq in range(SEQS):

        @pl.loop(1, 8)
        def _(j):
            col_copy(seq, j).wait_recv()

        mix_cols(seq)

        @pl.loop(1, 32)
        def _(j):
            grp_copy(seq, j).start()

        land[seq, grp_me] = ready[seq, grp_me]

    bank_load.wait()
    lanes = lax.broadcasted_iota(jnp.int32, (1, 128), 1)
    row = jnp.zeros((1, 128), jnp.float32)
    for seq in range(SEQS):

        @pl.loop(1, 32)
        def _(j):
            grp_copy(seq, j).wait_recv()

        chosen = index[seq]

        def add(i, carry):
            rows = pl.ds(pl.multiple_of(i * 8, 8), 8)
            value = land[seq, i]
            other = bank[chosen, rows]
            out[seq, rows] = value
            terms = (value * other, value * value, other * other)
            return tuple(total + term for total, term in zip(carry, terms))

        start = tuple(jnp.zeros((8, 512), jnp.float32) for _ in range(3))
        for kind, total in enumerate(lax.fori_loop(0, 32, add, start)):
            total = jnp.sum(jnp.sum(total, axis=1, keepdims=True), axis=0, keepdims=True)
            row = row + jnp.where(lanes == 2 * kind + seq, total, 0.0)

    mine[...] = row

    @pl.loop(1, 32)
    def _(j):
        red_copy(j).start()

    theirs[grp_me] = row

    @pl.loop(1, 32)
    def _(j):
        red_copy(j).wait_recv()

    row = lax.fori_loop(0, 32, lambda i, total: total + theirs[i], jnp.zeros((1, 128), jnp.float32))
    late[4] = row
    for step in range(3):
        late_copy(step).start()
    late[last_me] = row
    for step in range(3):
        late_copy(step).wait_recv()
    totals[...] = (late[0] + late[1]) + (late[2] + late[3])

    for seq in range(SEQS):

        @pl.loop(1, 8)
        def _(j):
            col_copy(seq, j).wait_send()

        @pl.loop(1, 32)
        def _(j):
            grp_copy(seq, j).wait_send()

    @pl.loop(1, 32)
    def _(j):
        red_copy(j).wait_send()

    for step in range(3):
        late_copy(step).wait_send()


def mixed_prints(sums, bank, bank_index):
    dma = pltpu.SemaphoreType.DMA
    vmem = pl.BlockSpec(memory_space=pltpu.VMEM)
    return pl.pallas_call(
        mix_kernel,
        out_shape=(
            jax.ShapeDtypeStruct((SEQS, 256, 512), jnp.float32),
            jax.ShapeDtypeStruct((1, 128), jnp.float32),
        ),
        in_specs=[
            pl.BlockSpec(memory_space=pl.ANY),
            pl.BlockSpec(memory_space=pl.ANY),
            pl.BlockSpec(memory_space=pltpu.SMEM),
        ],
        out_specs=(vmem, vmem),
        scratch_shapes=[
            pltpu.VMEM((SEQS, BLOCKS, 32, 2 * FEATS), jnp.float32),
            pltpu.VMEM((16, 256, 512), jnp.float32),
            pltpu.VMEM((512, 512), jnp.bfloat16),
            pltpu.VMEM((SEQS, 256, 512), jnp.float32),
            pltpu.VMEM((SEQS, 8, 32, 512), jnp.float32),
            pltpu.VMEM((SEQS, 32, 8, 512), jnp.float32),
            pltpu.VMEM((SEQS, 32, 8, 512), jnp.float32),
            pltpu.VMEM((1, 128), jnp.float32),
            pltpu.VMEM((32, 1, 128), jnp.float32),
            pltpu.VMEM((5, 1, 128), jnp.float32),
            dma((SEQS, 8)),
            dma((SEQS, 8)),
            dma((SEQS, 32)),
            dma((SEQS, 32)),
            dma((32,)),
            dma((32,)),
            dma((3,)),
            dma((3,)),
            dma((2,)),
        ],
        compiler_params=pltpu.CompilerParams(
            collective_id=1, has_side_effects=True, vmem_limit_bytes=67043328
        ),
    )(sums, bank, bank_index)


def body(activations, out_grads, token_mask, row_signs, col_signs, bank, bank_index):
    squared = float(D) * float(D)
    sums = gathered_products(
        activations,
        out_grads,
        row_signs.reshape(1, 256),
        col_signs.reshape(1, FEATS),
        token_mask,
    )
    prints, totals = mixed_prints(sums, bank, bank_index)
    cross, own, refsq = totals[0, 0:2], totals[0, 2:4], totals[0, 4:6]
    scores = D * (cross / squared) / jnp.sqrt((own / squared + 1e-06) * (refsq / squared + 1e-06))
    return prints, scores


def solution(mesh):
    split = Mesh(mesh.devices.reshape(4, 2, 2, 2, 4), EVERY)
    return jax.shard_map(
        body,
        mesh=split,
        in_specs=(
            P(None, TOK, COL),
            P(None, TOK, COL),
            P(None, TOK),
            P(TOK),
            P(COL),
            P(None, TOK, COL),
            P(),
        ),
        out_specs=(P(None, TOK, COL), P()),
        check_vma=False,
    )
```

```python
import functools
import math

import jax
import jax.numpy as jnp
from jax import lax
from jax.experimental import pallas as pl
from jax.experimental.pallas import tpu as pltpu
from jax.sharding import Mesh
from jax.sharding import PartitionSpec as P

D = 4096
TOK = ("tok_0", "tok_1", "tok_2")
COL = ("col_0", "col_1")
EVERY = ("tok_0", "tok_1", "tok_2", "col_0", "col_1")
MESH = pl.DeviceIdType.MESH

SEQS = 2
TOKENS = 1536
HALF = TOKENS // 2
FEATS = 512
BLOCKS = 4
UNITS = SEQS * BLOCKS * 2

ORDER = (
    ('run', 0, 0, 0),
    ('run', 1, 0, 0),
    ('core', 0, 0, 0),
    ('core', 1, 0, 0),
    ('half', 0, 0, 0),
    ('half', 1, 0, 0),
    ('spass', 0),
    ('rpass', 0),
    ('full', 0, 0, 0),
    ('full', 1, 0, 0),
    ('run', 0, 3, 0),
    ('run', 0, 0, 1),
    ('core', 0, 3, 0),
    ('run', 0, 3, 1),
    ('core', 0, 0, 1),
    ('run', 0, 1, 0),
    ('half', 0, 3, 0),
    ('core', 0, 3, 1),
    ('run', 0, 1, 1),
    ('half', 0, 0, 1),
    ('core', 0, 1, 0),
    ('core', 0, 1, 1),
    ('full', 0, 3, 0),
    ('half', 0, 3, 1),
    ('run', 0, 2, 0),
    ('spass', 1),
    ('full', 0, 0, 1),
    ('run', 0, 2, 1),
    ('half', 0, 1, 0),
    ('half', 0, 1, 1),
    ('core', 0, 2, 0),
    ('end', 0, 0, 0),
    ('end', 1, 0, 0),
    ('core', 0, 2, 1),
    ('end', 0, 3, 0),
    ('full', 0, 3, 1),
    ('full', 0, 1, 0),
    ('full', 0, 1, 1),
    ('half', 0, 2, 0),
    ('half', 0, 2, 1),
    ('rpass', 1),
    ('full', 0, 2, 0),
    ('full', 0, 2, 1),
    ('run', 1, 0, 1),
    ('end', 0, 0, 1),
    ('end', 0, 3, 1),
    ('core', 1, 0, 1),
    ('end', 0, 1, 0),
    ('end', 0, 1, 1),
    ('end', 0, 2, 0),
    ('half', 1, 0, 1),
    ('end', 0, 2, 1),
    ('run', 1, 3, 0),
    ('full', 1, 0, 1),
    ('run', 1, 3, 1),
    ('core', 1, 3, 0),
    ('run', 1, 1, 0),
    ('core', 1, 3, 1),
    ('run', 1, 1, 1),
    ('half', 1, 3, 0),
    ('core', 1, 1, 0),
    ('end', 1, 0, 1),
    ('half', 1, 3, 1),
    ('core', 1, 1, 1),
    ('full', 1, 3, 0),
    ('half', 1, 1, 0),
    ('run', 1, 2, 0),
    ('full', 1, 3, 1),
    ('run', 1, 2, 1),
    ('half', 1, 1, 1),
    ('core', 1, 2, 0),
    ('end', 1, 3, 0),
    ('full', 1, 1, 0),
    ('end', 1, 3, 1),
    ('core', 1, 2, 1),
    ('end', 1, 1, 0),
    ('full', 1, 1, 1),
    ('half', 1, 2, 0),
    ('half', 1, 2, 1),
    ('end', 1, 1, 1),
    ('full', 1, 2, 0),
    ('full', 1, 2, 1),
    ('end', 1, 2, 0),
    ('end', 1, 2, 1),
)


def hadamard_rows(first, rows, order):
    down = lax.broadcasted_iota(jnp.int32, (rows, order), 0) + first
    common_bits = jnp.bitwise_and(down, lax.broadcasted_iota(jnp.int32, (rows, order), 1))
    for shift in (8, 4, 2, 1):
        common_bits = jnp.bitwise_xor(common_bits, jnp.right_shift(common_bits, shift))
    return (1 - 2 * jnp.bitwise_and(common_bits, 1)).astype(jnp.float32)


def gather_kernel(
    acts,
    grads,
    row_bits,
    col_bits,
    mask,
    out,
    bits,
    walsh,
    tables,
    a_buf,
    m_buf,
    relay,
    part,
    core_in,
    x_half,
    x_full,
    y_in,
    load_sem,
    a_send,
    a_recv,
    m_send,
    m_recv,
    core_send,
    core_recv,
    xh_send,
    xh_recv,
    xf_send,
    xf_recv,
    y_send,
    y_recv,
    bit_load,
    bit_send,
    bit_recv,
):
    x = lax.axis_index("tok_0")
    y_lo = lax.axis_index("tok_1")
    core = lax.axis_index("tok_2")
    y_hi = lax.axis_index("col_0")
    z = lax.axis_index("col_1")
    y = y_hi * 2 + y_lo

    def at_y(value):
        value = lax.rem(value, 4)
        return (x, lax.rem(value, 2), core, lax.div(value, 2), z)

    x_next, x_prev, x_far = lax.rem(x + 1, 4), lax.rem(x + 3, 4), lax.rem(x + 2, 4)
    z_ids = ((x, y_lo, core, y_hi, lax.rem(z + 1, 4)), (x, y_lo, core, y_hi, lax.rem(z + 3, 4)))
    y_ids = (at_y(y + 1), at_y(y + 3))
    x_ids = ((x_next, y_lo, core, y_hi, z), (x_prev, y_lo, core, y_hi, z))
    core_id = (x, y_lo, 1 - core, y_hi, z)
    pair_id = (x, 1 - y_lo, core, y_hi, z)

    bit_own = pltpu.make_async_copy(row_bits, bits.at[core, x, y_lo], bit_load)
    m_own = [pltpu.make_async_copy(grads.at[seq], m_buf.at[seq, 0], load_sem.at[seq]) for seq in range(SEQS)]
    a_own = [pltpu.make_async_copy(acts.at[seq], a_buf.at[seq, 0], load_sem.at[2 + seq]) for seq in range(SEQS)]
    for copy in (bit_own, *m_own, *a_own):
        copy.start()

    barrier = pltpu.get_barrier_semaphore()
    partners = (*z_ids, *y_ids, *x_ids, core_id)
    for partner in partners:
        pl.semaphore_signal(barrier, inc=1, device_id=partner, device_id_type=MESH)
    pl.semaphore_wait(barrier, len(partners))

    def rows_of(half):
        return pl.ds(half * HALF, HALF)

    def remote(src, dst, send, recv, device):
        return pltpu.make_async_remote_copy(
            src_ref=src, dst_ref=dst, send_sem=send, recv_sem=recv, device_id=device, device_id_type=MESH
        )

    def ring_copy(seq, way, half, hop):
        slot = (3, 1)[way] if hop == 0 else 2
        index = (seq * 2 + way) * 3 + (2 if hop else half)
        src = acts.at[seq, rows_of(half)] if hop == 0 else a_buf.at[seq, (3, 1)[way], rows_of(half)]
        return remote(src, a_buf.at[seq, slot, rows_of(half)], a_send.at[index], a_recv.at[index], z_ids[way])

    def swap_copy(seq, way, hop):
        index = (seq * 2 + way) * 2 + hop
        src = relay.at[seq, way] if hop else m_buf.at[seq, 0, rows_of(way)]
        dst = m_buf.at[seq, 1, rows_of(way)] if hop else relay.at[seq, way]
        return remote(src, dst, m_send.at[index], m_recv.at[index], y_ids[way])

    sent = []

    def start(copy):
        copy.start()
        sent.append(copy)

    def ring_own(seq):
        for step in range(2):
            for way in range(2):
                start(ring_copy(seq, way, (way + step) % 2, 0))

    def ring_pass(seq):
        for way in range(2):
            ring_copy(seq, way, way, 0).wait_recv()
            start(ring_copy(seq, way, way, 1))

    def swap_own(seq):
        for way in range(2):
            start(swap_copy(seq, way, 0))

    def swap_pass(seq):
        for way in range(2):
            swap_copy(seq, way, 0).wait_recv()
            start(swap_copy(seq, way, 1))

    def swap_end(seq):
        for way in range(2):
            swap_copy(seq, way, 1).wait_recv()

    def ring_near(seq, way):
        ring_copy(seq, way, 1 - way, 0).wait_recv()

    def ring_far(seq):
        for way in range(2):
            ring_copy(seq, way, way, 1).wait_recv()

    def bit_copy(index, ref, device):
        return remote(ref, ref, bit_send.at[index], bit_recv.at[index], device)

    def share_bits():
        for way in range(2):
            start(bit_copy(1 + way, bits.at[core, x], x_ids[way]))
        for way in range(2):
            bit_copy(1 + way, bits.at[core, x], x_ids[way]).wait_recv()
        start(bit_copy(3, bits.at[core, x_prev], x_ids[0]))
        bit_copy(3, bits.at[core, x_prev], x_ids[0]).wait_recv()
        start(bit_copy(4, bits.at[core], core_id))

    def sign_tables():
        bit_copy(4, bits.at[core], core_id).wait_recv()

        @pl.loop(0, 8)
        def _(i):
            row = bits[lax.rem(i, 2), 2 * y_hi + lax.div(i, 4), lax.rem(lax.div(i, 2), 2)]
            signs = (2 * row - 1).astype(jnp.float32)
            tables[i] = (walsh[...] * signs).astype(jnp.bfloat16)

    def column_signs(seq):
        signs = (2 * col_bits[...] - 1).astype(jnp.float32).astype(jnp.bfloat16)

        @pl.loop(0, TOKENS // 32)
        def _(i):
            rows = pl.ds(pl.multiple_of(i * 32, 32), 32)
            m_buf[seq, 0, rows] = m_buf[seq, 0, rows] * signs

    core_sign = (1 - 2 * core).astype(jnp.float32)

    def compute(unit, seq, slot, m):
        block = lax.rem(z + slot, 4)
        counted = mask[seq : seq + 1, :].astype(jnp.float32).astype(jnp.bfloat16)

        @pl.loop(0, 2)
        def _(b):
            columns = pl.ds(pl.multiple_of(b * 256, 256), 256)
            rows_first = a_buf[seq, slot, :, columns].T * counted
            tile = jnp.dot(rows_first, m_buf[seq, m], preferred_element_type=jnp.float32)
            coarse = tile.astype(jnp.bfloat16)
            fine = (tile - coarse.astype(jnp.float32)).astype(jnp.bfloat16)
            table = tables[2 * block + b]
            mixed = jnp.dot(table, coarse, preferred_element_type=jnp.float32)
            mixed += jnp.dot(table, fine, preferred_element_type=jnp.float32)
            part[unit, b] = mixed

        @pl.loop(0, 16)
        def _(i):
            rows = pl.ds(pl.multiple_of(i * 16, 16), 16)
            low = part[unit, 0, rows]
            high = part[unit, 1, rows] * core_sign
            part[unit, 0, rows] = low + high
            part[unit, 1, rows] = low - high

        start(core_copy(unit))

    def core_copy(unit):
        return remote(part.at[unit, 1], core_in.at[unit], core_send.at[unit], core_recv.at[unit], core_id)

    def chunk(unit, x_of):
        return part.at[unit, 0, pl.ds(pl.multiple_of(x_of * 64, 64), 64)]

    def x_half_copy(unit, way):
        rows = pl.ds(pl.multiple_of(x_far * 64 + way * 32, 32), 32)
        index = unit * 2 + way
        return remote(
            part.at[unit, 0, rows], x_half.at[unit, way], xh_send.at[index], xh_recv.at[index], x_ids[way]
        )

    def x_full_copy(unit, way):
        index = unit * 2 + way
        src = chunk(unit, (x_next, x_prev)[way])
        return remote(src, x_full.at[unit, way], xf_send.at[index], xf_recv.at[index], x_ids[way])

    def y_copy(unit):
        rows = pl.ds(pl.multiple_of(x * 64 + (1 - y_lo) * 32, 32), 32)
        return remote(part.at[unit, 0, rows], y_in.at[unit], y_send.at[unit], y_recv.at[unit], pair_id)

    def sum_core(unit):
        core_copy(unit).wait_recv()

        def add(first, rows):
            @pl.loop(0, rows // 8)
            def _(i):
                there = pl.ds(pl.multiple_of(first + i * 8, 8), 8)
                part[unit, 0, there] += core_in[unit, there]

        add(x_far * 64, 64)
        for way in range(2):
            start(x_half_copy(unit, way))
        for other in (x_next, x_prev, x):
            add(other * 64, 64)

    def sum_half(unit):
        for way in range(2):
            x_half_copy(unit, way).wait_recv()
            first = (x_next, x_prev)[way] * 64 + way * 32

            @pl.loop(0, 4)
            def _(i):
                there = pl.ds(pl.multiple_of(first + i * 8, 8), 8)
                part[unit, 0, there] += x_half[unit, way, pl.ds(pl.multiple_of(i * 8, 8), 8)]

            start(x_full_copy(unit, way))

    def sum_full(unit):
        for way in range(2):
            x_full_copy(unit, way).wait_recv()

        @pl.loop(0, 8)
        def _(i):
            there = pl.ds(pl.multiple_of(x * 64 + i * 8, 8), 8)
            here = pl.ds(pl.multiple_of(i * 8, 8), 8)
            part[unit, 0, there] += x_full[unit, 0, here] + x_full[unit, 1, here]

        start(y_copy(unit))

    def finish(unit, seq, slot, m):
        block = lax.rem(z + slot, 4)
        columns = pl.ds(pl.multiple_of(lax.rem(m + y_hi, 2) * FEATS, FEATS), FEATS)
        y_copy(unit).wait_recv()

        @pl.loop(0, 4)
        def _(i):
            here = pl.ds(pl.multiple_of(i * 8, 8), 8)
            there = pl.ds(pl.multiple_of(x * 64 + y_lo * 32 + i * 8, 8), 8)
            out[seq, block, here, columns] = part[unit, 0, there] + y_in[unit, here]

    ring_own(0)
    walsh[...] = hadamard_rows(0, 256, 256)
    bit_own.wait()
    start(bit_copy(0, bits.at[core, x, y_lo], pair_id))
    m_own[0].wait()
    column_signs(0)
    swap_own(0)
    bit_copy(0, bits.at[core, x, y_lo], pair_id).wait_recv()
    share_bits()
    m_own[1].wait()
    column_signs(1)
    for copy in a_own:
        copy.wait()
    sign_tables()

    here = {("a", 0, 0), ("a", 1, 0), ("m", 0, 0), ("m", 1, 0)}

    def once(key, wait):
        if key not in here:
            here.add(key)
            wait()

    for step, *rest in ORDER:
        if step == "spass":
            swap_pass(rest[0])
            if rest[0] == 0:
                swap_own(1)
            continue
        if step == "rpass":
            ring_pass(rest[0])
            if rest[0] == 0:
                ring_own(1)
            continue
        seq, slot, m = rest
        unit = (seq * BLOCKS + slot) * 2 + m
        if step == "run":
            if slot == 2:
                once(("a", seq, 2), lambda seq=seq: ring_far(seq))
            else:
                once(("a", seq, slot), lambda seq=seq, slot=slot: ring_near(seq, 0 if slot == 3 else 1))
            once(("m", seq, m), lambda seq=seq: swap_end(seq))
            compute(unit, seq, slot, m)
        elif step == "core":
            sum_core(unit)
        elif step == "half":
            sum_half(unit)
        elif step == "full":
            sum_full(unit)
        else:
            finish(unit, seq, slot, m)
    for copy in sent:
        copy.wait_send()


def gathered_products(acts, grads, row_bits, col_bits, mask):
    dma = pltpu.SemaphoreType.DMA
    return pl.pallas_call(
        gather_kernel,
        out_shape=jax.ShapeDtypeStruct((SEQS, BLOCKS, 32, 2 * FEATS), jnp.float32),
        in_specs=[
            pl.BlockSpec(memory_space=pl.ANY),
            pl.BlockSpec(memory_space=pl.ANY),
            pl.BlockSpec(memory_space=pl.ANY),
            pl.BlockSpec(memory_space=pltpu.VMEM),
            pl.BlockSpec(memory_space=pltpu.VMEM),
        ],
        out_specs=pl.BlockSpec(memory_space=pltpu.VMEM),
        scratch_shapes=[
            pltpu.VMEM((2, 4, 2, 1, 256), jnp.int32),
            pltpu.VMEM((256, 256), jnp.float32),
            pltpu.VMEM((8, 256, 256), jnp.bfloat16),
            pltpu.VMEM((SEQS, BLOCKS, TOKENS, FEATS), jnp.bfloat16),
            pltpu.VMEM((SEQS, 2, TOKENS, FEATS), jnp.bfloat16),
            pltpu.VMEM((SEQS, 2, HALF, FEATS), jnp.bfloat16),
            pltpu.VMEM((UNITS, 2, 256, FEATS), jnp.float32),
            pltpu.VMEM((UNITS, 256, FEATS), jnp.float32),
            pltpu.VMEM((UNITS, 2, 32, FEATS), jnp.float32),
            pltpu.VMEM((UNITS, 2, 64, FEATS), jnp.float32),
            pltpu.VMEM((UNITS, 32, FEATS), jnp.float32),
            dma((4,)),
            dma((12,)),
            dma((12,)),
            dma((8,)),
            dma((8,)),
            dma((UNITS,)),
            dma((UNITS,)),
            dma((2 * UNITS,)),
            dma((2 * UNITS,)),
            dma((2 * UNITS,)),
            dma((2 * UNITS,)),
            dma((UNITS,)),
            dma((UNITS,)),
            dma,
            dma((5,)),
            dma((5,)),
        ],
        compiler_params=pltpu.CompilerParams(
            collective_id=0, has_side_effects=True, vmem_limit_bytes=67043328
        ),
    )(acts, grads, row_bits, col_bits, mask)


def mix_kernel(
    sums_there,
    bank_there,
    index,
    out,
    totals,
    sums,
    bank,
    walsh,
    work,
    got,
    ready,
    land,
    mine,
    theirs,
    late,
    col_send,
    col_recv,
    grp_send,
    grp_recv,
    red_send,
    red_recv,
    late_send,
    late_recv,
    load_sem,
):
    x = lax.axis_index("tok_0")
    y_lo = lax.axis_index("tok_1")
    core = lax.axis_index("tok_2")
    y_hi = lax.axis_index("col_0")
    z = lax.axis_index("col_1")
    col_me = y_hi * 4 + z
    grp_me = x * 8 + y_lo * 4 + z

    def col_peer(j):
        there_y = lax.rem(y_hi + lax.div(j, 4), 2)
        there_z = lax.rem(z + j, 4)
        return there_y * 4 + there_z, (x, y_lo, core, there_y, there_z)

    def grp_peer(j):
        there_x = lax.rem(x + lax.div(j, 8), 4)
        there_y = lax.rem(y_lo + lax.div(j, 4), 2)
        there_z = lax.rem(z + j, 4)
        return there_x * 8 + there_y * 4 + there_z, (there_x, there_y, core, y_hi, there_z)

    core_id = (x, y_lo, 1 - core, y_hi, z)
    far_id = (x, y_lo, core, 1 - y_hi, z)
    last_ids = (far_id, core_id, (x, y_lo, 1 - core, 1 - y_hi, z))
    last_me = y_hi * 2 + core

    sums_load = pltpu.make_async_copy(sums_there, sums, load_sem.at[0])
    bank_load = pltpu.make_async_copy(bank_there, bank, load_sem.at[1])
    sums_load.start()
    bank_load.start()
    barrier = pltpu.get_barrier_semaphore()

    @pl.loop(1, 8)
    def _(j):
        pl.semaphore_signal(barrier, inc=1, device_id=col_peer(j)[1], device_id_type=MESH)

    @pl.loop(1, 32)
    def _(j):
        pl.semaphore_signal(barrier, inc=1, device_id=grp_peer(j)[1], device_id_type=MESH)

    for partner in last_ids[1:]:
        pl.semaphore_signal(barrier, inc=1, device_id=partner, device_id_type=MESH)

    @pl.loop(0, 8)
    def _(i):
        rows = pl.ds(pl.multiple_of(i * 64, 64), 64)
        walsh[rows] = hadamard_rows(i * 64, 64, 512).astype(jnp.bfloat16)

    def remote(src, dst, send, recv, device):
        return pltpu.make_async_remote_copy(
            src_ref=src, dst_ref=dst, send_sem=send, recv_sem=recv, device_id=device, device_id_type=MESH
        )

    def piece(peer):
        return pl.ds(pl.multiple_of(peer * 32, 32), 32)

    def col_copy(seq, j):
        peer, device = col_peer(j)
        return remote(
            work.at[seq, piece(peer)], got.at[seq, col_me], col_send.at[seq, j], col_recv.at[seq, j], device
        )

    def grp_copy(seq, j):
        peer, device = grp_peer(j)
        return remote(
            ready.at[seq, peer], land.at[seq, grp_me], grp_send.at[seq, j], grp_recv.at[seq, j], device
        )

    def red_copy(j):
        return remote(mine, theirs.at[grp_me], red_send.at[j], red_recv.at[j], grp_peer(j)[1])

    def late_copy(step):
        return remote(late.at[4], late.at[last_me], late_send.at[step], late_recv.at[step], last_ids[step])

    def pair(low, high):
        return low + high, low - high

    def four(values):
        a, b = pair(values[0], values[2])
        c, d = pair(values[1], values[3])
        first, second = pair(a, c)
        third, fourth = pair(b, d)
        return first, second, third, fourth

    def mix_local(seq):
        @pl.loop(0, 4)
        def _(q):
            rows = pl.ds(pl.multiple_of(q * 8, 8), 8)
            for half in range(2):
                columns = slice(half * 256, half * 256 + 256)
                upper = slice(512 + half * 256, 768 + half * 256)
                left = four([sums[seq, a, rows, columns] for a in range(4)])
                right = four([sums[seq, a, rows, upper] for a in range(4)])
                for a in range(4):
                    low, high = pair(left[a], right[a])
                    work[seq, pl.ds(pl.multiple_of(q * 32 + a * 8, 8), 8), columns] = low
                    work[seq, pl.ds(pl.multiple_of(128 + q * 32 + a * 8, 8), 8), columns] = high

        values = work[seq]
        coarse = values.astype(jnp.bfloat16)
        fine = (values - coarse.astype(jnp.float32)).astype(jnp.bfloat16)
        mixed = jnp.dot(coarse, walsh[...], preferred_element_type=jnp.float32)
        mixed += jnp.dot(fine, walsh[...], preferred_element_type=jnp.float32)
        work[seq] = mixed * (1.0 / D)

    def mix_cols(seq):
        @pl.loop(0, 4)
        def _(o):
            for part in range(2):
                columns = slice(part * 256, part * 256 + 256)
                rows = pl.ds(pl.multiple_of(o * 8, 8), 8)
                left = four([got[seq, src, rows, columns] for src in range(4)])
                right = four([got[seq, 4 + src, rows, columns] for src in range(4)])
                for c in range(4):
                    low, high = pair(left[c], right[c])
                    ready[seq, o * 4 + c, :, columns] = low
                    ready[seq, 16 + o * 4 + c, :, columns] = high

    sums_load.wait()
    for seq in range(SEQS):
        mix_local(seq)
        if seq == 0:
            pl.semaphore_wait(barrier, 40)

        @pl.loop(1, 8)
        def _(j):
            col_copy(seq, j).start()

        got[seq, col_me] = work[seq, piece(col_me)]

    for seq in range(SEQS):

        @pl.loop(1, 8)
        def _(j):
            col_copy(seq, j).wait_recv()

        mix_cols(seq)

        @pl.loop(1, 32)
        def _(j):
            grp_copy(seq, j).start()

        land[seq, grp_me] = ready[seq, grp_me]

    bank_load.wait()
    lanes = lax.broadcasted_iota(jnp.int32, (1, 128), 1)
    row = jnp.zeros((1, 128), jnp.float32)
    for seq in range(SEQS):

        @pl.loop(1, 32)
        def _(j):
            grp_copy(seq, j).wait_recv()

        chosen = index[seq]

        def add(i, carry):
            rows = pl.ds(pl.multiple_of(i * 8, 8), 8)
            value = land[seq, i]
            other = bank[chosen, rows]
            out[seq, rows] = value
            terms = (value * other, value * value, other * other)
            return tuple(total + term for total, term in zip(carry, terms))

        start = tuple(jnp.zeros((8, 512), jnp.float32) for _ in range(3))
        for kind, total in enumerate(lax.fori_loop(0, 32, add, start)):
            total = jnp.sum(jnp.sum(total, axis=1, keepdims=True), axis=0, keepdims=True)
            row = row + jnp.where(lanes == 2 * kind + seq, total, 0.0)

    mine[...] = row

    @pl.loop(1, 32)
    def _(j):
        red_copy(j).start()

    theirs[grp_me] = row

    @pl.loop(1, 32)
    def _(j):
        red_copy(j).wait_recv()

    row = lax.fori_loop(0, 32, lambda i, total: total + theirs[i], jnp.zeros((1, 128), jnp.float32))
    late[4] = row
    for step in range(3):
        late_copy(step).start()
    late[last_me] = row
    for step in range(3):
        late_copy(step).wait_recv()
    totals[...] = (late[0] + late[1]) + (late[2] + late[3])

    for seq in range(SEQS):

        @pl.loop(1, 8)
        def _(j):
            col_copy(seq, j).wait_send()

        @pl.loop(1, 32)
        def _(j):
            grp_copy(seq, j).wait_send()

    @pl.loop(1, 32)
    def _(j):
        red_copy(j).wait_send()

    for step in range(3):
        late_copy(step).wait_send()


def mixed_prints(sums, bank, bank_index):
    dma = pltpu.SemaphoreType.DMA
    vmem = pl.BlockSpec(memory_space=pltpu.VMEM)
    return pl.pallas_call(
        mix_kernel,
        out_shape=(
            jax.ShapeDtypeStruct((SEQS, 256, 512), jnp.float32),
            jax.ShapeDtypeStruct((1, 128), jnp.float32),
        ),
        in_specs=[
            pl.BlockSpec(memory_space=pl.ANY),
            pl.BlockSpec(memory_space=pl.ANY),
            pl.BlockSpec(memory_space=pltpu.SMEM),
        ],
        out_specs=(vmem, vmem),
        scratch_shapes=[
            pltpu.VMEM((SEQS, BLOCKS, 32, 2 * FEATS), jnp.float32),
            pltpu.VMEM((16, 256, 512), jnp.float32),
            pltpu.VMEM((512, 512), jnp.bfloat16),
            pltpu.VMEM((SEQS, 256, 512), jnp.float32),
            pltpu.VMEM((SEQS, 8, 32, 512), jnp.float32),
            pltpu.VMEM((SEQS, 32, 8, 512), jnp.float32),
            pltpu.VMEM((SEQS, 32, 8, 512), jnp.float32),
            pltpu.VMEM((1, 128), jnp.float32),
            pltpu.VMEM((32, 1, 128), jnp.float32),
            pltpu.VMEM((5, 1, 128), jnp.float32),
            dma((SEQS, 8)),
            dma((SEQS, 8)),
            dma((SEQS, 32)),
            dma((SEQS, 32)),
            dma((32,)),
            dma((32,)),
            dma((3,)),
            dma((3,)),
            dma((2,)),
        ],
        compiler_params=pltpu.CompilerParams(
            collective_id=1, has_side_effects=True, vmem_limit_bytes=67043328
        ),
    )(sums, bank, bank_index)


def body(activations, out_grads, token_mask, row_signs, col_signs, bank, bank_index):
    squared = float(D) * float(D)
    sums = gathered_products(
        activations,
        out_grads,
        row_signs.reshape(1, 256),
        col_signs.reshape(1, FEATS),
        token_mask,
    )
    prints, totals = mixed_prints(sums, bank, bank_index)
    cross, own, refsq = totals[0, 0:2], totals[0, 2:4], totals[0, 4:6]
    scores = D * (cross / squared) / jnp.sqrt((own / squared + 1e-06) * (refsq / squared + 1e-06))
    return prints, scores


def solution(mesh):
    split = Mesh(mesh.devices.reshape(4, 2, 2, 2, 4), EVERY)
    return jax.shard_map(
        body,
        mesh=split,
        in_specs=(
            P(None, TOK, COL),
            P(None, TOK, COL),
            P(None, TOK),
            P(TOK),
            P(COL),
            P(None, TOK, COL),
            P(),
        ),
        out_specs=(P(None, TOK, COL), P()),
        check_vma=False,
    )
```
